128 devices in a mesh: head: 8 (over z, x_hi), seq: 16 (over x_lo, y, core).
Axes of the slice: x: 4 (x_hi: 2, x_lo: 2; x = x_hi * 2 + x_lo), y: 4, z: 4, core: 2. Of those that a mesh axis runs over, the one named last changes fastest.
Arguments:
- keys: bfloat16 [2, 8192, 5120], P(None, 'seq', 'head'), may hold values from -6 to 6
- values: bfloat16 [2, 8192, 5120], P(None, 'seq', 'head'), may hold values from -6 to 6
- step_rates: float32 [2, 8, 8192], P(None, 'head', 'seq'), may hold values from 0.05 to 1
- queries: bfloat16 [8192, 5120], P('seq', 'head'), may hold values from -6 to 6
- first_weight: bfloat16 [8, 640, 640], P('head'), may hold values from -0.25 to 0.25
- third_weight: bfloat16 [8, 640, 640], P('head'), may hold values from -0.25 to 0.25
- second_weight: bfloat16 [8, 640, 640], P('head'), may hold values from -0.25 to 0.25
- out_weight: bfloat16 [5120, 5120], P('head'), may hold values from -0.078125 to 0.078125
- live_counts: int32 [3, 16], P(None, 'seq'), may hold values from 256 to 512
Outputs:
- mixed: bfloat16 [8192, 5120], P('seq', 'head')
The draws below stay inside these ranges and needn't reach their ends.
Inputs may be any that keep to these rules, and one draw needn't show every extreme that they name: `live_counts`: the live rows of a shard are its first ones.
All inputs are finite; a program needn't handle non-finite values.
Results may differ from the reference program's by a relative error of at most 0.023.
Values may be sent and summed in bfloat16 or wider, within the bound.
No kernel may reach another device: no remote copies, remote signals or barrier semaphores. Data moves between devices by JAX's collectives and lax.ppermute only.
A program may use at most 128 MiB of HBM per device.

```python
import math
import jax
import jax.numpy as jnp
from jax import lax

DH = 640
FH = 640
TOK_DEV = 512
GROUPS = 2
NS_ITERS = 3
HEADS = 8
D = 5120
TOKENS = 8192
SHARDS = 16


def set_ends(values, rng, low, largest):
    index_at = [jax.random.randint(jax.random.fold_in(rng, axis), (), 0, length) for axis, length in enumerate(values.shape)]
    widest = values.shape.index(max(values.shape))
    neighbour = index_at[:widest] + [(index_at[widest] + 1) % values.shape[widest]] + index_at[widest + 1:]
    return values.at[tuple(index_at)].set(low).at[tuple(neighbour)].set(largest)


def block_scale(rng, shape, split, low, high):
    level = 1.0
    for position, blocks in split:
        steps = jax.random.uniform(jax.random.fold_in(jax.random.fold_in(rng, 6), position), (blocks,), jnp.float32, low / len(split), high / len(split))
        level = level * jnp.repeat(jnp.exp(steps), shape[position] // blocks).reshape((-1,) + (1,) * (len(shape) - 1 - position))
    return level


def gaussian(stream_key, extent, scale, most, split=(), held_as=jnp.bfloat16):
    values = scale * jax.random.normal(stream_key, extent, jnp.float32)
    if split:
        values = values * block_scale(stream_key, extent, split, -0.22, 0.18)
    return jnp.clip(values, -most, most).astype(held_as)


def setup_inputs(seed: int = 0) -> dict:
    arg_keys = jax.random.split(jax.random.key(seed), 10)
    return {
        "keys": gaussian(arg_keys[0], (GROUPS, TOKENS, D), 1.0, 6.0, ((1, 16), (2, 8))),
        "values": gaussian(arg_keys[1], (GROUPS, TOKENS, D), 1.0, 6.0, ((1, 16), (2, 8))),
        "step_rates": jnp.clip(jnp.exp(math.log(1.0) - 2.9957323 * jax.random.uniform(arg_keys[2], (GROUPS, HEADS, TOKENS), jnp.float32) ** block_scale(arg_keys[2], (GROUPS, HEADS, TOKENS), ((1, 8), (2, 16)), -0.2, 0.2)), 0.05, 1.0),
        "queries": gaussian(arg_keys[3], (TOKENS, D), 1.0, 6.0, ((0, 16), (1, 8))),
        "first_weight": gaussian(arg_keys[4], (HEADS, DH, FH), DH ** -0.5, 0.25, ((0, 8),)),
        "third_weight": gaussian(arg_keys[5], (HEADS, DH, FH), DH ** -0.5, 0.25, ((0, 8),)),
        "second_weight": gaussian(arg_keys[6], (HEADS, FH, DH), FH ** -0.5, 0.25, ((0, 8),)),
        "out_weight": gaussian(arg_keys[7], (D, D), D ** -0.5, 0.078125, ((0, 8),)),
        "live_counts": set_ends(jax.random.randint(arg_keys[8], (GROUPS + 1, SHARDS), TOK_DEV // 2, TOK_DEV + 1), jax.random.fold_in(arg_keys[8], 1), TOK_DEV // 2, TOK_DEV).astype(jnp.int32),
    }


coef_a = 3.4445
coef_b = -4.775
coef_c = 2.0315
step_size = 0.5

def fast_grads(inputs, targets, scaling, first, third, second):
    first_pre = jnp.dot(inputs, first, preferred_element_type=jnp.float32)
    third_pre = jnp.dot(inputs, third, preferred_element_type=jnp.float32)
    sigmoid = jax.nn.sigmoid(first_pre)
    swish = first_pre * sigmoid
    hidden = (swish * third_pre).astype(jnp.bfloat16)
    weighted = (targets.astype(jnp.float32) * scaling[:, None]).astype(jnp.bfloat16)
    grad_second = jnp.dot(hidden.T, weighted, preferred_element_type=jnp.float32)
    back = jnp.dot(weighted, second.T, preferred_element_type=jnp.float32)
    back_first = (back * third_pre * sigmoid * (1.0 + first_pre * (1.0 - sigmoid))).astype(jnp.bfloat16)
    back_third = (back * swish).astype(jnp.bfloat16)
    grad_first = jnp.dot(inputs.T, back_first, preferred_element_type=jnp.float32)
    grad_third = jnp.dot(inputs.T, back_third, preferred_element_type=jnp.float32)
    return (grad_first, grad_third, grad_second)

def orthogonal(gradient):
    scale = jnp.sqrt(jnp.sum(gradient * gradient)) + 1e-06
    current = (gradient / scale).astype(jnp.bfloat16)
    for index in range(NS_ITERS):
        gram_wide = jnp.dot(current, current.T, preferred_element_type=jnp.float32)
        gram_low = gram_wide.astype(jnp.bfloat16)
        poly = (coef_b * gram_wide + coef_c * jnp.dot(gram_low, gram_low, preferred_element_type=jnp.float32)).astype(jnp.bfloat16)
        current = (coef_a * current.astype(jnp.float32) + jnp.dot(poly, current, preferred_element_type=jnp.float32)).astype(jnp.bfloat16)
    return current

def renewed(weight, gradient):
    old = weight.astype(jnp.float32)
    fresh = old + step_size * orthogonal(gradient).astype(jnp.float32)
    ratio = jnp.sqrt(lax.optimization_barrier(jnp.mean(old * old, axis=0)) + 1e-06) / jnp.sqrt(lax.optimization_barrier(jnp.mean(fresh * fresh, axis=0)) + 1e-06)
    return (fresh * ratio[None, :]).astype(jnp.bfloat16)

def applied(inputs, first, third, second, live):
    first_pre = jnp.dot(inputs, first, preferred_element_type=jnp.float32)
    third_pre = jnp.dot(inputs, third, preferred_element_type=jnp.float32)
    hidden = (jax.nn.silu(first_pre) * third_pre).astype(jnp.bfloat16)
    result = jnp.dot(hidden, second, preferred_element_type=jnp.float32)
    return (result * live[:, None]).astype(jnp.bfloat16)

def reference(keys, values, step_rates, queries, first_weight, third_weight, second_weight, out_weight, live_counts):
    indices = jnp.arange(TOKENS).astype(jnp.int32)
    positions = indices % TOK_DEV
    owners = indices // TOK_DEV
    outputs = []
    for head in range(HEADS):
        lower = head * DH
        totals = None
        for group in range(GROUPS):
            live = (positions < live_counts[group][owners]).astype(jnp.float32)
            scaling = live * step_rates[group, head]
            parts = fast_grads(keys[group][:, lower:lower + DH], values[group][:, lower:lower + DH], scaling, first_weight[head], third_weight[head], second_weight[head])
            totals = parts if totals is None else tuple((a + b for a, b in zip(totals, parts)))
        new_first = renewed(first_weight[head], totals[0])
        new_third = renewed(third_weight[head], totals[1])
        new_second = renewed(second_weight[head], totals[2])
        live_query = (positions < live_counts[GROUPS][owners]).astype(jnp.float32)
        outputs.append(applied(queries[:, lower:lower + DH], new_first, new_third, new_second, live_query))
    merged = jnp.concatenate(outputs, axis=1)
    return jnp.dot(merged, out_weight, preferred_element_type=jnp.float32).astype(jnp.bfloat16)
```

```python
import jax
import jax.numpy as jnp
from jax import lax
from jax.experimental import pallas as pl
from jax.experimental.pallas import tpu as pltpu
from jax.sharding import Mesh
from jax.sharding import PartitionSpec as P

NS_ITERS = 3
HEAD = ("z", "xh")
SEQ = ("xl", "y", "c")
CHIPS = ("xl", "y")


coef_a = 3.4445
coef_b = -4.775
coef_c = 2.0315
step_size = 0.5

BF = jnp.bfloat16
F32 = jnp.float32


def sds(shape, dtype):
    return jax.ShapeDtypeStruct(shape, dtype)


def vmem(count):
    return [pl.BlockSpec(memory_space=pltpu.VMEM)] * count


def smem():
    return pl.BlockSpec(memory_space=pltpu.SMEM)


def call(body, outs, in_specs, scratch=(), flops=0, limit=32):
    return pl.pallas_call(
        body,
        out_shape=outs,
        in_specs=in_specs,
        out_specs=jax.tree.map(lambda _: pl.BlockSpec(memory_space=pltpu.VMEM), outs),
        scratch_shapes=scratch,
        compiler_params=pltpu.CompilerParams(vmem_limit_bytes=limit << 20),
        cost_estimate=pl.CostEstimate(flops=flops, bytes_accessed=4 << 20, transcendentals=0),
    )


def dot(left, right):
    return jnp.dot(left, right, preferred_element_type=F32)


def dot_tn(left, right):
    return lax.dot_general(left, right, (((0,), (0,)), ((), ())), preferred_element_type=F32)


def dot_nt(left, right):
    return lax.dot_general(left, right, (((1,), (1,)), ((), ())), preferred_element_type=F32)


def grads_body(
    meta, keys, values, rates, first, third, second,
    mine, other, half, half_other,
    hidden_s, weighted_s, bm_s, bo_s,
):
    core0 = meta[0] == 0
    groups, rows, wide = keys.shape
    tile = 256
    per = rows // tile
    lanes = 128
    for group in range(groups):
        for part in range(per):
            base = group * rows + part * tile
            block = pl.ds(base, tile)
            span = pl.ds(part * tile, tile)
            spot = lax.broadcasted_iota(jnp.int32, (1, tile), 1) + part * tile
            row = jnp.where(spot < meta[1 + group], rates[group, :, span], 0.0)
            scale = jnp.broadcast_to(row, (lanes, tile)).T
            scale = jnp.concatenate([scale] * (wide // lanes), axis=1)
            weighted = (values[group, span, :].astype(F32) * scale).astype(BF)
            weighted_s[block, :] = weighted
            k = keys[group, span, :]
            first_pre = dot(k, first[...])
            third_pre = dot(k, third[...])
            sig = 1.0 / (1.0 + jnp.exp(-first_pre))
            swish = first_pre * sig
            hidden_s[block, :] = (swish * third_pre).astype(BF)
            back = dot_nt(weighted, second[...])
            back_first = (back * third_pre * sig * (1.0 + first_pre * (1.0 - sig))).astype(BF)
            back_third = (back * swish).astype(BF)
            bm_s[block, :] = jnp.where(core0, back_first, back_third)
            bo_s[block, :] = jnp.where(core0, back_third, back_first)
    k_all = keys[...].reshape(groups * rows, wide)
    mine[...] = dot_tn(k_all, bm_s[...])
    other[...] = dot_tn(k_all, bo_s[...]).astype(BF)
    low = wide // 2
    total = dot_tn(hidden_s[...], weighted_s[...])
    half[...] = jnp.where(core0, total[:low], total[low:])
    half_other[...] = jnp.where(core0, total[low:], total[:low]).astype(BF)


def grads(meta, keys, values, rates, first, third, second):
    groups, rows, wide = keys.shape
    total = groups * rows
    return call(
        grads_body,
        (
            sds((wide, wide), F32),
            sds((wide, wide), BF),
            sds((wide // 2, wide), F32),
            sds((wide // 2, wide), BF),
        ),
        [smem()] + vmem(6),
        [pltpu.VMEM((total, wide), BF)] * 4,
        flops=6 * 2 * total * wide * wide,
        limit=44,
    )(meta, keys, values, rates, first, third, second)


OFFSETS = ((0, 0), (0, 1), (0, 3), (0, 2), (1, 0), (1, 1), (1, 3), (1, 2))


def chip_perm(offset, ylen):
    dx, dy = offset
    return [
        (x * ylen + y, ((x + dx) % 2) * ylen + (y + dy) % ylen) for x in range(2) for y in range(ylen)
    ]


def fold_body(meta, mine, got, *rest):
    outs, full = rest[:-1], rest[-1]
    full[...] = mine[...] + got[...].astype(F32)
    rows = outs[0].shape[0]
    for index, out in enumerate(outs):
        out[...] = full[pl.ds(pl.multiple_of(meta[index] * rows, 8), rows), :].astype(out.dtype)


def fold(table, mine, got):
    rows, wide = mine.shape
    part = rows // len(OFFSETS)
    outs = (sds((part, wide), F32),) + (sds((part, wide), BF),) * (len(OFFSETS) - 1)
    return call(
        fold_body, outs, [smem()] + vmem(2), [pltpu.VMEM((rows, wide), F32)], flops=1 << 27, limit=12
    )(table, mine, got)


def exchange(parts, ylen):
    return [
        lax.ppermute(part, CHIPS, chip_perm(offset, ylen)) for part, offset in zip(parts, OFFSETS[1:])
    ]


def summed(own, got):
    total = own
    for part in got:
        total = total + part.astype(F32)
    return total.astype(BF)


def ns_core(full, x_s):
    grad = full[...]
    scale = jnp.sqrt(jnp.sum(grad * grad)) + 1e-06
    x_s[...] = (grad / scale).astype(BF)

    def step(_, carry):
        x = x_s[...]
        gram = dot_nt(x, x)
        low = gram.astype(BF)
        poly = (coef_b * gram + coef_c * dot(low, low)).astype(BF)
        x_s[...] = (coef_a * x.astype(F32) + dot(poly, x)).astype(BF)
        return carry

    lax.fori_loop(0, NS_ITERS, step, 0)


def renew(old, x_s, out):
    fresh = old + step_size * x_s[...].astype(F32)
    ratio = jnp.sqrt(jnp.mean(old * old, axis=0, keepdims=True) + 1e-06) / jnp.sqrt(
        jnp.mean(fresh * fresh, axis=0, keepdims=True) + 1e-06
    )
    out[...] = (fresh * ratio).astype(BF)


def ns_pair_body(meta, *refs):
    chunks, (first, third, out, full, x_s) = refs[:8], refs[8:]
    rows = chunks[0].shape[0]
    for index, chunk in enumerate(chunks):
        full[pl.ds(pl.multiple_of(meta[1 + index] * rows, 8), rows), :] = chunk[...].astype(F32)
    ns_core(full, x_s)
    old = jnp.where(meta[0] == 0, first[...], third[...]).astype(F32)
    renew(old, x_s, out)


def ns_half_body(meta, own, got, second, out, full, x_s):
    half, wide = own.shape
    rows = half // 8
    core = meta[0]
    for index in range(8):
        spot = meta[1 + index] * rows
        piece = pl.ds(index * rows, rows)
        full[pl.ds(pl.multiple_of(core * half + spot, 8), rows), :] = own[piece, :].astype(F32)
        full[pl.ds(pl.multiple_of((1 - core) * half + spot, 8), rows), :] = got[piece, :].astype(F32)
    ns_core(full, x_s)
    renew(second[...].astype(F32), x_s, out)


def ns_call(body, count, wide):
    return call(
        body,
        sds((wide, wide), BF),
        [smem()] + vmem(count),
        [pltpu.VMEM((wide, wide), F32), pltpu.VMEM((wide, wide), BF)],
        flops=9 * 2 * wide**3,
        limit=24,
    )


def apply_body(meta, queries, mine, got, second, out):
    core0 = meta[0] == 0
    rows, wide = out.shape
    tile = 256
    for part in range(rows // tile):
        span = pl.ds(part * tile, tile)
        q = queries[span, :]
        a = dot(q, mine[...])
        b = dot(q, got[...])
        first_pre = jnp.where(core0, a, b)
        third_pre = jnp.where(core0, b, a)
        hidden = (first_pre / (1.0 + jnp.exp(-first_pre)) * third_pre).astype(BF)
        spot = lax.broadcasted_iota(jnp.int32, (tile, wide), 0) + part * tile
        out[span, :] = jnp.where(spot < meta[1], dot(hidden, second[...]), 0.0).astype(BF)


def apply(meta, queries, mine, got, second):
    rows, wide = queries.shape
    return call(
        apply_body, sds((rows, wide), BF), [smem()] + vmem(4), flops=6 * rows * wide * wide, limit=16
    )(meta, queries, mine, got, second)


def project(table, head_out, out_weight, picks, layout, dtypes):
    rows, wide = head_out.shape
    count = len(picks)

    def body(meta, x, *refs):
        blocks, outs = refs[:count], refs[count:]
        products = [dot(x[...], block[...]) for block in blocks]
        for out, value in zip(outs, layout(products)):
            out[...] = value.astype(out.dtype)

    shapes = jax.eval_shape(layout, [sds((rows, wide), F32)] * count)
    outs = tuple(sds(shape.shape, dtype) for shape, dtype in zip(shapes, dtypes))
    grid_spec = pltpu.PrefetchScalarGridSpec(
        num_scalar_prefetch=1,
        grid=(1,),
        in_specs=[pl.BlockSpec((rows, wide), lambda i, t: (0, 0))]
        + [pl.BlockSpec((wide, wide), lambda i, t, pick=pick: (0, t[pick])) for pick in picks],
        out_specs=tuple(pl.BlockSpec(out.shape, lambda i, t: (0, 0)) for out in outs),
    )
    return pl.pallas_call(
        body,
        grid_spec=grid_spec,
        out_shape=outs,
        compiler_params=pltpu.CompilerParams(vmem_limit_bytes=24 << 20),
        cost_estimate=pl.CostEstimate(
            flops=2 * count * rows * wide * wide, bytes_accessed=2 << 20, transcendentals=0
        ),
    )(table, head_out, *([out_weight] * count))


def turn(count, by):
    return [(index, (index + by) % count) for index in range(count)]


def mixed_sum(head_out, out_weight, zlen):
    z = lax.axis_index("z")
    x = lax.axis_index("xh")

    def block(dz, dx):
        return ((z + dz) % zlen) * 2 + (x + dx) % 2

    table = jnp.stack(
        [block(2, 1), block(2, 0), block(1, 1), block(3, 1), block(1, 0), block(3, 0), block(0, 1), block(0, 0)]
    ).astype(jnp.int32)
    half = head_out.shape[0] // 2
    up = lambda v: lax.ppermute(v, "z", turn(zlen, 1))
    down = lambda v: lax.ppermute(v, "z", turn(zlen, zlen - 1))
    over = lambda v: lax.ppermute(v, "xh", turn(2, 1))

    def wide(*values):
        return sum(value.astype(F32) for value in values)

    far_top, far_low = project(
        table, head_out, out_weight, (0,), lambda p: [p[0][:half], p[0][half:]], (BF, BF)
    )
    far_top = up(far_top)
    far_low = down(far_low)
    cross, hold_up, hold_down = project(
        table,
        head_out,
        out_weight,
        (2, 3),
        lambda p: [jnp.concatenate([p[1][:half], p[0][half:]]), p[0][:half], p[1][half:]],
        (BF, F32, F32),
    )
    cross = over(cross)
    same_top, same_low = project(
        table, head_out, out_weight, (1,), lambda p: [p[0][:half], p[0][half:]], (BF, BF)
    )
    same_top = up(same_top)
    same_low = down(same_low)
    next_up, next_down, next_over, own = project(
        table, head_out, out_weight, (4, 5, 6, 7), lambda p: p, (F32, F32, F32, F32)
    )
    by_up = up(wide(hold_up, far_top).astype(BF))
    by_down = down(wide(hold_down, far_low).astype(BF))
    to_up = wide(next_up, jnp.concatenate([same_top, cross[half:]])).astype(BF)
    to_down = wide(next_down, jnp.concatenate([cross[:half], same_low])).astype(BF)
    from_low = up(to_up)
    from_high = down(to_down)
    to_over = wide(next_over, jnp.concatenate([by_up, by_down])).astype(BF)
    from_over = over(to_over)
    return wide(own, from_low, from_high, from_over).astype(BF)


def on_device(
    keys, values, step_rates, queries, first_weight, third_weight, second_weight, out_weight,
    live_counts, ylen, zlen,
):
    core = lax.axis_index("c").astype(jnp.int32)
    xl = lax.axis_index("xl")
    y = lax.axis_index("y")
    wide = keys.shape[2]
    first, third, second = first_weight[0], third_weight[0], second_weight[0]
    counts = live_counts[:, 0]
    group_count = keys.shape[0]
    meta = jnp.concatenate([core[None], counts])
    to_chip = jnp.stack([((xl + dx) % 2) * ylen + (y + dy) % ylen for dx, dy in OFFSETS]).astype(jnp.int32)
    from_chip = jnp.stack([((xl + dx) % 2) * ylen + (y - dy) % ylen for dx, dy in OFFSETS]).astype(jnp.int32)
    ns_meta = jnp.concatenate([core[None], from_chip])
    swap = lambda v: lax.ppermute(v, "c", turn(2, 1))

    mine, other, half, half_other = grads(meta, keys, values, step_rates, first, third, second)
    pair = fold(to_chip, mine, swap(other))
    halves = fold(to_chip, half, swap(half_other))
    pair_own = summed(pair[0], exchange(pair[1:], ylen))
    pair_all = [pair_own] + exchange([pair_own] * 7, ylen)
    half_own = summed(halves[0], exchange(halves[1:], ylen))
    half_all = jnp.concatenate([half_own] + exchange([half_own] * 7, ylen))
    half_got = swap(half_all)
    new_mine = ns_call(ns_pair_body, 10, wide)(ns_meta, *pair_all, first, third)
    new_got = swap(new_mine)
    new_second = ns_call(ns_half_body, 3, wide)(ns_meta, half_all, half_got, second)
    query_meta = jnp.stack([core, counts[group_count]])
    head_out = apply(query_meta, queries, new_mine, new_got, new_second)
    return mixed_sum(head_out, out_weight, zlen)


def solution(mesh):
    xlen, ylen, zlen = 2, 4, 4
    split = Mesh(mesh.devices.reshape(zlen, 2, xlen, ylen, 2), HEAD + SEQ)
    in_specs = (
        P(None, SEQ, HEAD),
        P(None, SEQ, HEAD),
        P(None, HEAD, SEQ),
        P(SEQ, HEAD),
        P(HEAD, None, None),
        P(HEAD, None, None),
        P(HEAD, None, None),
        P(HEAD, None),
        P(None, SEQ),
    )

    def body(*args):
        return on_device(*args, ylen, zlen)

    return jax.shard_map(
        body, mesh=split, in_specs=in_specs, out_specs=P(SEQ, HEAD), check_vma=False
    )
```

```python
import jax
import jax.numpy as jnp
from jax import lax
from jax.experimental import pallas as pl
from jax.experimental.pallas import tpu as pltpu
from jax.sharding import Mesh
from jax.sharding import PartitionSpec as P

NS_ITERS = 3
HEAD = ("z", "xh")
SEQ = ("xl", "y", "c")
CHIPS = ("xl", "y")


coef_a = 3.4445
coef_b = -4.775
coef_c = 2.0315
step_size = 0.5

BF = jnp.bfloat16
F32 = jnp.float32


def sds(shape, dtype):
    return jax.ShapeDtypeStruct(shape, dtype)


def vmem(count):
    return [pl.BlockSpec(memory_space=pltpu.VMEM)] * count


def smem():
    return pl.BlockSpec(memory_space=pltpu.SMEM)


def call(body, outs, in_specs, scratch=(), flops=0, limit=32):
    return pl.pallas_call(
        body,
        out_shape=outs,
        in_specs=in_specs,
        out_specs=jax.tree.map(lambda _: pl.BlockSpec(memory_space=pltpu.VMEM), outs),
        scratch_shapes=scratch,
        compiler_params=pltpu.CompilerParams(vmem_limit_bytes=limit << 20),
        cost_estimate=pl.CostEstimate(flops=flops, bytes_accessed=4 << 20, transcendentals=0),
    )


def dot(left, right):
    return jnp.dot(left, right, preferred_element_type=F32)


def dot_tn(left, right):
    return lax.dot_general(left, right, (((0,), (0,)), ((), ())), preferred_element_type=F32)


def dot_nt(left, right):
    return lax.dot_general(left, right, (((1,), (1,)), ((), ())), preferred_element_type=F32)


def core_is_first():
    return lax.axis_index("c") == 0


def grads_body(
    counts, keys_h, values_h, rates_h, first_h, third_h, second_h,
    mine, other, half, half_other,
    keys, values, rates, first, third, second, hidden_s, weighted_s, bm_s, bo_s, sems,
):
    core0 = core_is_first()
    groups, rows, wide = keys_h.shape
    copies = {}

    def fetch(name, source, target):
        copies[name] = pltpu.make_async_copy(source, target, sems.at[len(copies)])
        copies[name].start()

    fetch("first", first_h.at[0], first)
    fetch("k0", keys_h.at[0], keys.at[pl.ds(0, rows)])
    fetch("third", third_h.at[0], third)
    fetch("rates", rates_h, rates)
    fetch("v0", values_h.at[0], values.at[pl.ds(0, rows)])
    fetch("second", second_h.at[0], second)
    for group in range(1, groups):
        fetch(f"k{group}", keys_h.at[group], keys.at[pl.ds(group * rows, rows)])
        fetch(f"v{group}", values_h.at[group], values.at[pl.ds(group * rows, rows)])

    def ready(*names):
        for name in names:
            if name in copies:
                copies.pop(name).wait()

    tile = 256
    lanes = 128
    for group in range(groups):
        for part in range(rows // tile):
            block = pl.ds(group * rows + part * tile, tile)
            ready("first", f"k{group}", "third")
            k = keys[block, :]
            first_pre = dot(k, first[...])
            third_pre = dot(k, third[...])
            ready("rates", f"v{group}", "second")
            spot = lax.broadcasted_iota(jnp.int32, (1, tile), 1) + part * tile
            row = jnp.where(spot < counts[group, 0], rates[group, :, pl.ds(part * tile, tile)], 0.0)
            scale = jnp.broadcast_to(row, (lanes, tile)).T
            scale = jnp.concatenate([scale] * (wide // lanes), axis=1)
            weighted = (values[block, :].astype(F32) * scale).astype(BF)
            weighted_s[block, :] = weighted
            sig = 1.0 / (1.0 + jnp.exp(-first_pre))
            swish = first_pre * sig
            hidden_s[block, :] = (swish * third_pre).astype(BF)
            back = dot_nt(weighted, second[...])
            back_first = (back * third_pre * sig * (1.0 + first_pre * (1.0 - sig))).astype(BF)
            back_third = (back * swish).astype(BF)
            bm_s[block, :] = jnp.where(core0, back_first, back_third)
            bo_s[block, :] = jnp.where(core0, back_third, back_first)
    mine[...] = dot_tn(keys[...], bm_s[...])
    other[...] = dot_tn(keys[...], bo_s[...]).astype(BF)
    low = wide // 2
    total = dot_tn(hidden_s[...], weighted_s[...])
    half[...] = jnp.where(core0, total[:low], total[low:])
    half_other[...] = jnp.where(core0, total[low:], total[:low]).astype(BF)


def grads(counts, keys, values, rates, first, third, second):
    groups, rows, wide = keys.shape
    total = groups * rows
    tokens = pltpu.VMEM((total, wide), BF)
    weight = pltpu.VMEM((wide, wide), BF)
    return call(
        grads_body,
        (
            sds((wide, wide), F32),
            sds((wide, wide), BF),
            sds((wide // 2, wide), F32),
            sds((wide // 2, wide), BF),
        ),
        [smem()] + [pl.BlockSpec(memory_space=pltpu.HBM)] * 6,
        [tokens, tokens, pltpu.VMEM(rates.shape, F32), weight, weight, weight]
        + [tokens] * 4
        + [pltpu.SemaphoreType.DMA((4 + 2 * groups,))],
        flops=6 * 2 * total * wide * wide,
        limit=57,
    )(counts, keys, values, rates, first, third, second)


def fold_body(mine, got, half, half_got, out):
    chips = out.shape[0]
    rows = mine.shape[0] // chips
    less = half.shape[0] // chips
    for index in range(chips):
        span = pl.ds(index * rows, rows)
        out[index, pl.ds(0, rows), :] = (mine[span, :] + got[span, :].astype(F32)).astype(BF)
        span = pl.ds(index * less, less)
        out[index, pl.ds(rows, less), :] = (half[span, :] + half_got[span, :].astype(F32)).astype(BF)


def fold(mine, got, half, half_got, chips):
    wide = mine.shape[1]
    out = sds((chips, (mine.shape[0] + half.shape[0]) // chips, wide), BF)
    return call(fold_body, out, vmem(4), flops=1 << 27, limit=10)(mine, got, half, half_got)


def spread_body(parts, out):
    total = parts[0].astype(F32)
    for index in range(1, parts.shape[0]):
        total = total + parts[index].astype(F32)
    for index in range(parts.shape[0]):
        out[index] = total.astype(BF)


def spread(parts):
    return call(spread_body, sds(parts.shape, BF), vmem(1), flops=1 << 27, limit=10)(parts)


def trade(parts):
    return lax.all_to_all(parts, CHIPS, 0, 0)


def ns_core(full, x_s):
    grad = full[...]
    scale = jnp.sqrt(jnp.sum(grad * grad)) + 1e-06
    x_s[...] = (grad / scale).astype(BF)

    def step(_, carry):
        x = x_s[...]
        gram = dot_nt(x, x)
        low = gram.astype(BF)
        poly = (coef_b * gram + coef_c * dot(low, low)).astype(BF)
        x_s[...] = (coef_a * x.astype(F32) + dot(poly, x)).astype(BF)
        return carry

    lax.fori_loop(0, NS_ITERS, step, 0)


def renew(old, x_s, out):
    fresh = old + step_size * x_s[...].astype(F32)
    ratio = jnp.sqrt(jnp.mean(old * old, axis=0, keepdims=True) + 1e-06) / jnp.sqrt(
        jnp.mean(fresh * fresh, axis=0, keepdims=True) + 1e-06
    )
    out[...] = (fresh * ratio).astype(BF)


def ns_pair_body(totals, first, third, out, full, x_s):
    chips = totals.shape[0]
    rows = full.shape[0] // chips
    for index in range(chips):
        full[pl.ds(index * rows, rows), :] = totals[index, pl.ds(0, rows), :].astype(F32)
    ns_core(full, x_s)
    old = jnp.where(core_is_first(), first[...], third[...]).astype(F32)
    renew(old, x_s, out)


def ns_half_body(own, got, second, out, full, x_s):
    core0 = core_is_first()
    chips, rows, _ = own.shape
    low = chips * rows
    for index in range(chips):
        a = own[index].astype(F32)
        b = got[index].astype(F32)
        full[pl.ds(index * rows, rows), :] = jnp.where(core0, a, b)
        full[pl.ds(low + index * rows, rows), :] = jnp.where(core0, b, a)
    ns_core(full, x_s)
    renew(second[...].astype(F32), x_s, out)


def ns_call(body, count, wide):
    return call(
        body,
        sds((wide, wide), BF),
        vmem(count),
        [pltpu.VMEM((wide, wide), F32), pltpu.VMEM((wide, wide), BF)],
        flops=9 * 2 * wide**3,
        limit=24,
    )


def project_call(body, table, operands, out_weight, picks, outs, flops):
    wide = out_weight.shape[0]
    whole = lambda shape: pl.BlockSpec(shape, lambda i, t: (0,) * len(shape))
    grid_spec = pltpu.PrefetchScalarGridSpec(
        num_scalar_prefetch=1,
        grid=(1,),
        in_specs=[
            smem() if operand.dtype == jnp.int32 else whole(operand.shape) for operand in operands
        ]
        + [pl.BlockSpec((wide, wide), lambda i, t, pick=pick: (0, t[pick])) for pick in picks],
        out_specs=tuple(whole(out.shape) for out in outs),
    )
    return pl.pallas_call(
        body,
        grid_spec=grid_spec,
        out_shape=outs,
        compiler_params=pltpu.CompilerParams(vmem_limit_bytes=24 << 20),
        cost_estimate=pl.CostEstimate(flops=flops, bytes_accessed=2 << 20, transcendentals=0),
    )(table, *operands, *([out_weight] * len(picks)))


def apply_body(meta, counts, queries, mine, got, second, far, next_up, next_down, out, *outs):
    core0 = core_is_first()
    rows, wide = out.shape
    limit = counts[counts.shape[0] - 1, 0]
    tile = rows // 2
    far_top, far_low, cross, hold_up, hold_down = outs
    for part, far_out, hold in ((0, far_top, hold_up), (1, far_low, hold_down)):
        span = pl.ds(part * tile, tile)
        q = queries[span, :]
        a = dot(q, mine[...])
        b = dot(q, got[...])
        first_pre = jnp.where(core0, a, b)
        third_pre = jnp.where(core0, b, a)
        hidden = (first_pre / (1.0 + jnp.exp(-first_pre)) * third_pre).astype(BF)
        spot = lax.broadcasted_iota(jnp.int32, (tile, wide), 0) + part * tile
        head = jnp.where(spot < limit, dot(hidden, second[...]), 0.0).astype(BF)
        out[span, :] = head
        far_out[...] = dot(head, far[...]).astype(BF)
        cross_block, hold_block = (next_down, next_up) if part == 0 else (next_up, next_down)
        cross[span, :] = dot(head, cross_block[...]).astype(BF)
        hold[...] = dot(head, hold_block[...])


def project_body(count):
    def body(meta, x, *refs):
        for block, out in zip(refs[:count], refs[count:]):
            out[...] = dot(x[...], block[...]).astype(out.dtype)

    return body


def halves_body(meta, x, block, top, low):
    half = top.shape[0]
    top[...] = dot(x[pl.ds(0, half), :], block[...]).astype(BF)
    low[...] = dot(x[pl.ds(half, half), :], block[...]).astype(BF)


def turn(count, by):
    return [(index, (index + by) % count) for index in range(count)]


def mixed_sum(counts, queries, new_mine, new_got, new_second, out_weight, zlen):
    z = lax.axis_index("z")
    x = lax.axis_index("xh")

    def block(dz, dx):
        return ((z + dz) % zlen) * 2 + (x + dx) % 2

    table = jnp.stack(
        [block(2, 1), block(2, 0), block(1, 1), block(3, 1), block(1, 0), block(3, 0), block(0, 1), block(0, 0)]
    ).astype(jnp.int32)
    rows, cols = queries.shape
    half = rows // 2
    one = 2 * rows * cols * cols
    up = lambda v: lax.ppermute(v, "z", turn(zlen, 1))
    down = lambda v: lax.ppermute(v, "z", turn(zlen, zlen - 1))
    over = lambda v: lax.ppermute(v, "xh", turn(2, 1))

    def wide(*values):
        return sum(value.astype(F32) for value in values)

    full, part = (rows, cols), (half, cols)
    head_out, far_top, far_low, cross, hold_up, hold_down = project_call(
        apply_body,
        table,
        (counts, queries, new_mine, new_got, new_second),
        out_weight,
        (0, 2, 3),
        (sds(full, BF), sds(part, BF), sds(part, BF), sds(full, BF), sds(part, F32), sds(part, F32)),
        6 * one,
    )
    far_top = up(far_top)
    far_low = down(far_low)
    cross = over(cross)
    same_top, same_low = project_call(
        halves_body, table, (head_out,), out_weight, (1,), (sds(part, BF), sds(part, BF)), one
    )
    same_top = up(same_top)
    same_low = down(same_low)
    next_up, next_down, next_over, own = project_call(
        project_body(4), table, (head_out,), out_weight, (4, 5, 6, 7), (sds(full, F32),) * 4, 4 * one
    )
    by_up = up(wide(hold_up, far_top).astype(BF))
    by_down = down(wide(hold_down, far_low).astype(BF))
    to_up = wide(next_up, jnp.concatenate([same_top, cross[half:]])).astype(BF)
    to_down = wide(next_down, jnp.concatenate([cross[:half], same_low])).astype(BF)
    from_low = up(to_up)
    from_high = down(to_down)
    to_over = wide(next_over, jnp.concatenate([by_up, by_down])).astype(BF)
    from_over = over(to_over)
    return wide(own, from_low, from_high, from_over).astype(BF)


def on_device(
    keys, values, step_rates, queries, first_weight, third_weight, second_weight, out_weight,
    live_counts, ylen, zlen,
):
    wide = keys.shape[2]
    first, third, second = first_weight[0], third_weight[0], second_weight[0]
    swap = lambda v: lax.ppermute(v, "c", turn(2, 1))

    mine, other, half, half_other = grads(
        live_counts, keys, values, step_rates, first_weight, third_weight, second_weight
    )
    folded = fold(mine, swap(other), half, swap(half_other), 2 * ylen)
    totals = trade(spread(trade(folded)))
    rows = wide // (2 * ylen)
    half_own = totals[:, rows:]
    half_got = swap(half_own)
    new_mine = ns_call(ns_pair_body, 3, wide)(totals, first, third)
    new_got = swap(new_mine)
    new_second = ns_call(ns_half_body, 3, wide)(half_own, half_got, second)
    return mixed_sum(live_counts, queries, new_mine, new_got, new_second, out_weight, zlen)


def solution(mesh):
    xlen, ylen, zlen = 2, 4, 4
    split = Mesh(mesh.devices.reshape(zlen, 2, xlen, ylen, 2), HEAD + SEQ)
    in_specs = (
        P(None, SEQ, HEAD),
        P(None, SEQ, HEAD),
        P(None, HEAD, SEQ),
        P(SEQ, HEAD),
        P(HEAD, None, None),
        P(HEAD, None, None),
        P(HEAD, None, None),
        P(HEAD, None),
        P(None, SEQ),
    )

    def body(*args):
        return on_device(*args, ylen, zlen)

    return jax.shard_map(
        body, mesh=split, in_specs=in_specs, out_specs=P(SEQ, HEAD), check_vma=False
    )
```

```python
import jax
import jax.numpy as jnp
from jax import lax
from jax.experimental import pallas as pl
from jax.experimental.pallas import tpu as pltpu
from jax.sharding import Mesh
from jax.sharding import PartitionSpec as P


NS_ITERS = 3
GRADS_LIMIT = 52
PAIR_LIMIT = 30
HALF_LIMIT = 40
HEAD = ("z", "xh")
SEQ = ("xl", "y", "c")
CHIPS = ("xl", "y")


coef_a = 3.4445
coef_b = -4.775
coef_c = 2.0315
step_size = 0.5

BF = jnp.bfloat16
F32 = jnp.float32


def sds(shape, dtype):
    return jax.ShapeDtypeStruct(shape, dtype)


def vmem(count):
    return [pl.BlockSpec(memory_space=pltpu.VMEM)] * count


def smem():
    return pl.BlockSpec(memory_space=pltpu.SMEM)


def far_spec():
    return pl.BlockSpec(memory_space=pltpu.HBM)


def call(body, outs, in_specs, scratch=(), flops=0, limit=32):
    return pl.pallas_call(
        body,
        out_shape=outs,
        in_specs=in_specs,
        out_specs=jax.tree.map(lambda _: pl.BlockSpec(memory_space=pltpu.VMEM), outs),
        scratch_shapes=scratch,
        compiler_params=pltpu.CompilerParams(vmem_limit_bytes=limit << 20),
        cost_estimate=pl.CostEstimate(flops=flops, bytes_accessed=4 << 20, transcendentals=0),
    )


def dot(left, right):
    return jnp.dot(left, right, preferred_element_type=F32)


def dot_tn(left, right):
    return lax.dot_general(left, right, (((0,), (0,)), ((), ())), preferred_element_type=F32)


def dot_nt(left, right):
    return lax.dot_general(left, right, (((1,), (1,)), ((), ())), preferred_element_type=F32)


def core_is_first():
    return lax.axis_index("c") == 0


def grads_body(
    keys_h, values_h, rates, first_h, third_h, second_h,
    mine, other, half, half_other,
    keys, values, first, third, second, hidden_s, weighted_s, bm_s, bo_s, sems,
):
    core0 = core_is_first()
    groups, rows, wide = keys_h.shape
    copies = {}

    def fetch(name, source, target):
        copies[name] = pltpu.make_async_copy(source, target, sems.at[len(copies)])
        copies[name].start()

    fetch("first", first_h.at[0], first)
    fetch("k0", keys_h.at[0], keys.at[pl.ds(0, rows)])
    fetch("third", third_h.at[0], third)
    fetch("v0", values_h.at[0], values.at[pl.ds(0, rows)])
    fetch("second", second_h.at[0], second)
    for group in range(1, groups):
        fetch(f"k{group}", keys_h.at[group], keys.at[pl.ds(group * rows, rows)])
        fetch(f"v{group}", values_h.at[group], values.at[pl.ds(group * rows, rows)])

    def ready(*names):
        for name in names:
            if name in copies:
                copies.pop(name).wait()

    tile = 256
    lanes = 128
    for group in range(groups):
        for part in range(rows // tile):
            block = pl.ds(group * rows + part * tile, tile)
            ready("first", f"k{group}", "third")
            k = keys[block, :]
            first_pre = dot(k, first[...])
            third_pre = dot(k, third[...])
            ready(f"v{group}", "second")
            row = rates[group, :, pl.ds(part * tile, tile)]
            scale = jnp.broadcast_to(row, (lanes, tile)).T
            scale = jnp.concatenate([scale] * (wide // lanes), axis=1)
            weighted = (values[block, :].astype(F32) * scale).astype(BF)
            weighted_s[block, :] = weighted
            sig = 1.0 / (1.0 + jnp.exp(-first_pre))
            swish = first_pre * sig
            hidden_s[block, :] = (swish * third_pre).astype(BF)
            back = dot_nt(weighted, second[...])
            back_first = (back * third_pre * sig * (1.0 + first_pre * (1.0 - sig))).astype(BF)
            back_third = (back * swish).astype(BF)
            bm_s[block, :] = jnp.where(core0, back_first, back_third)
            bo_s[block, :] = jnp.where(core0, back_third, back_first)
    mine[...] = dot_tn(keys[...], bm_s[...]).astype(BF)
    other[...] = dot_tn(keys[...], bo_s[...]).astype(BF)
    low = wide // 2
    total = dot_tn(hidden_s[...], weighted_s[...])
    half[...] = jnp.where(core0, total[:low], total[low:]).astype(BF)
    half_other[...] = jnp.where(core0, total[low:], total[:low]).astype(BF)


def grads(keys, values, rates, first, third, second):
    groups, rows, wide = keys.shape
    total = groups * rows
    tokens = pltpu.VMEM((total, wide), BF)
    weight = pltpu.VMEM((wide, wide), BF)
    return call(
        grads_body,
        (
            sds((wide, wide), BF),
            sds((wide, wide), BF),
            sds((wide // 2, wide), BF),
            sds((wide // 2, wide), BF),
        ),
        [far_spec(), far_spec(), vmem(1)[0]] + [far_spec()] * 3,
        [tokens, tokens, weight, weight, weight]
        + [tokens] * 4
        + [pltpu.SemaphoreType.DMA((3 + 2 * groups,))],
        flops=6 * 2 * total * wide * wide,
        limit=GRADS_LIMIT,
    )(keys, values, rates, first, third, second)


def fold_body(mine, got, half, half_got, out):
    chips = out.shape[0]
    rows = mine.shape[0] // chips
    less = half.shape[0] // chips
    for index in range(chips):
        for own, more, base, size in ((mine, got, 0, rows), (half, half_got, rows, less)):
            span = pl.ds(index * size, size)
            total = own[span, :].astype(F32) + more[span, :].astype(F32)
            out[index, pl.ds(base, size), :] = total.astype(BF)


def fold(mine, got, half, half_got, chips):
    wide = mine.shape[1]
    out = sds((chips, (mine.shape[0] + half.shape[0]) // chips, wide), BF)
    return call(fold_body, out, vmem(4), flops=1 << 27, limit=10)(mine, got, half, half_got)


def spread_body(parts, out):
    total = parts[0].astype(F32)
    for index in range(1, parts.shape[0]):
        total = total + parts[index].astype(F32)
    for index in range(parts.shape[0]):
        out[index] = total.astype(BF)


def spread(parts):
    return call(spread_body, sds(parts.shape, BF), vmem(1), flops=1 << 27, limit=10)(parts)


def trade(parts):
    return lax.all_to_all(parts, CHIPS, 0, 0)


def ns_core(full, x_s):
    grad = full[...]
    scale = jnp.sqrt(jnp.sum(grad * grad)) + 1e-06
    x_s[...] = (grad / scale).astype(BF)

    def step(_, carry):
        x = x_s[...]
        gram = dot_nt(x, x)
        low = gram.astype(BF)
        poly = (coef_b * gram + coef_c * dot(low, low)).astype(BF)
        x_s[...] = (coef_a * x.astype(F32) + dot(poly, x)).astype(BF)
        return carry

    lax.fori_loop(0, NS_ITERS, step, 0)


def renew(old, x_s, out):
    fresh = old + step_size * x_s[...].astype(F32)
    ratio = jnp.sqrt(jnp.mean(old * old, axis=0, keepdims=True) + 1e-06) / jnp.sqrt(
        jnp.mean(fresh * fresh, axis=0, keepdims=True) + 1e-06
    )
    out[...] = (fresh * ratio).astype(BF)


def begin(copies, sems):
    started = [
        pltpu.make_async_copy(source, target, sems.at[index])
        for index, (source, target) in enumerate(copies)
    ]
    for copy in started:
        copy.start()
    return started


def ns_pair_body(totals, first, third, second_h, queries_h, out, second, queries, full, x_s, sems):
    copies = begin([(second_h.at[0], second), (queries_h, queries)], sems)
    chips = totals.shape[0]
    rows = full.shape[0] // chips
    for index in range(chips):
        full[pl.ds(index * rows, rows), :] = totals[index, pl.ds(0, rows), :].astype(F32)
    ns_core(full, x_s)
    old = jnp.where(core_is_first(), first[...], third[...]).astype(F32)
    renew(old, x_s, out)
    for copy in copies:
        copy.wait()


def ns_half_body(places, zlen, own, got, second, weight_h, out, *refs):
    count = len(places)
    blocks, (full, x_s, sems) = refs[:count], refs[count:]
    z = lax.axis_index("z")
    x = lax.axis_index("xh")
    wide = out.shape[1]
    columns = [lax.rem(z + dz, zlen) * 2 + lax.rem(x + dx, 2) for dz, dx in places]
    copies = begin(
        [
            (weight_h.at[:, pl.ds(pl.multiple_of(column * wide, 128), wide)], block)
            for column, block in zip(columns, blocks)
        ],
        sems,
    )
    core0 = core_is_first()
    chips = own.shape[0]
    low = wide // 2
    rows = low // chips
    part = pl.ds(own.shape[1] - rows, rows)
    for index in range(chips):
        a = own[index, part, :].astype(F32)
        b = got[index, part, :].astype(F32)
        full[pl.ds(index * rows, rows), :] = jnp.where(core0, a, b)
        full[pl.ds(low + index * rows, rows), :] = jnp.where(core0, b, a)
    ns_core(full, x_s)
    renew(second[...].astype(F32), x_s, out)
    for copy in copies:
        copy.wait()


def ns_scratch(wide, copies):
    return [
        pltpu.VMEM((wide, wide), F32),
        pltpu.VMEM((wide, wide), BF),
        pltpu.SemaphoreType.DMA((copies,)),
    ]


def ns_pair(totals, first, third, second, queries):
    wide = first.shape[1]
    weight = sds((wide, wide), BF)
    return call(
        ns_pair_body,
        (weight, weight, sds(queries.shape, BF)),
        vmem(3) + [far_spec()] * 2,
        ns_scratch(wide, 2),
        flops=9 * 2 * wide**3,
        limit=PAIR_LIMIT,
    )(totals, first, third, second, queries)


def ns_half(places, zlen, own, got, second, out_weight):
    wide = second.shape[1]

    def body(*refs):
        ns_half_body(places, zlen, *refs)

    return call(
        body,
        (sds((wide, wide), BF),) * (1 + len(places)),
        vmem(3) + [far_spec()],
        ns_scratch(wide, len(places)),
        flops=9 * 2 * wide**3,
        limit=HALF_LIMIT,
    )(own, got, second, out_weight)


def apply_body(counts, queries, mine, got, second, far, same, next_up, next_down, out, *outs):
    core0 = core_is_first()
    rows, wide = out.shape
    limit = counts[0, counts.shape[1] - 1]
    tile = rows // 2
    far_top, far_low, cross, same_top, same_low, hold_up, hold_down = outs
    for part in range(2):
        far_out, same_out, hold = (
            (far_top, same_top, hold_up) if part == 0 else (far_low, same_low, hold_down)
        )
        span = pl.ds(part * tile, tile)
        q = queries[span, :]
        a = dot(q, mine[...])
        b = dot(q, got[...])
        first_pre = jnp.where(core0, a, b)
        third_pre = jnp.where(core0, b, a)
        hidden = (first_pre / (1.0 + jnp.exp(-first_pre)) * third_pre).astype(BF)
        spot = lax.broadcasted_iota(jnp.int32, (tile, wide), 0) + part * tile
        head = jnp.where(spot < limit, dot(hidden, second[...]), 0.0).astype(BF)
        out[span, :] = head
        far_out[...] = dot(head, far[...]).astype(BF)
        cross_block, hold_block = (next_down, next_up) if part == 0 else (next_up, next_down)
        cross[span, :] = dot(head, cross_block[...]).astype(BF)
        same_out[...] = dot(head, same[...]).astype(BF)
        hold[...] = dot(head, hold_block[...])


def project_body(x, *refs):
    count = len(refs) // 2
    for block, out in zip(refs[:count], refs[count:]):
        out[...] = dot(x[...], block[...])


def turn(count, by):
    return [(index, (index + by) % count) for index in range(count)]


PLACES = ((2, 1), (2, 0), (1, 1), (3, 1), (1, 0), (3, 0), (0, 1), (0, 0))


def mixed_sum(counts, queries, new_mine, new_got, new_second, blocks, zlen):
    rows, cols = queries.shape
    half = rows // 2
    one = 2 * rows * cols * cols

    def send(value, axis, by):
        return lax.ppermute(value, axis, turn({"z": zlen, "xh": 2}[axis], by))

    def wide(*values):
        return sum(value.astype(F32) for value in values)

    full, part = (rows, cols), (half, cols)
    head_out, far_top, far_low, cross, same_top, same_low, hold_up, hold_down = call(
        apply_body,
        (sds(full, BF), sds(part, BF), sds(part, BF), sds(full, BF))
        + (sds(part, BF), sds(part, BF), sds(part, F32), sds(part, F32)),
        [smem()] + vmem(8),
        flops=7 * one,
        limit=24,
    )(counts, queries, new_mine, new_got, new_second, *blocks[:4])
    far_top = send(far_top, "z", 1)
    far_low = send(far_low, "z", zlen - 1)
    cross = send(cross, "xh", 1)
    same_top = send(same_top, "z", 1)
    same_low = send(same_low, "z", zlen - 1)
    next_up, next_down, next_over, own = call(
        project_body, (sds(full, F32),) * 4, vmem(5), flops=4 * one, limit=24
    )(head_out, *blocks[4:])
    by_up = send(wide(hold_up, far_top).astype(BF), "z", 1)
    by_down = send(wide(hold_down, far_low).astype(BF), "z", zlen - 1)
    to_up = wide(next_up, jnp.concatenate([same_top, cross[half:]])).astype(BF)
    to_down = wide(next_down, jnp.concatenate([cross[:half], same_low])).astype(BF)
    from_low = send(to_up, "z", 1)
    from_high = send(to_down, "z", zlen - 1)
    over_top = send(add_rows(next_over, by_up, 0), "xh", 1)
    over_low = send(add_rows(next_over, by_down, half), "xh", 1)
    from_over = jnp.concatenate([over_top, over_low])
    return wide(own, from_low, from_high, from_over).astype(BF)


def add_rows(full, more, start):
    rows = more.shape[0]

    def body(a, b, out):
        out[...] = (a[pl.ds(start, rows), :] + b[...].astype(F32)).astype(BF)

    return call(body, sds(more.shape, BF), vmem(2), flops=1 << 24, limit=8)(full, more)


def on_device(
    keys, values, step_rates, queries, first_weight, third_weight, second_weight, out_weight,
    live_counts, ylen, zlen,
):
    first, third = first_weight[0], third_weight[0]
    swap = lambda v: lax.ppermute(v, "c", turn(2, 1))

    counts = live_counts.T
    groups, rows, _ = keys.shape
    live = jnp.arange(rows, dtype=jnp.int32)[None, None, :] < live_counts[:groups, :, None]
    scales = jnp.where(live, step_rates, 0.0)
    mine, other, half, half_other = grads(
        keys, values, scales, first_weight, third_weight, second_weight
    )
    totals = trade(spread(trade(fold(mine, swap(other), half, swap(half_other), 2 * ylen))))
    totals_got = swap(totals)
    new_mine, second, near_queries = ns_pair(totals, first, third, second_weight, queries)
    new_got = swap(new_mine)
    new_second, *blocks = ns_half(PLACES, zlen, totals, totals_got, second, out_weight)
    return mixed_sum(counts, near_queries, new_mine, new_got, new_second, blocks, zlen)


def solution(mesh):
    xlen, ylen, zlen = 2, 4, 4
    split = Mesh(mesh.devices.reshape(zlen, 2, xlen, ylen, 2), HEAD + SEQ)
    in_specs = (
        P(None, SEQ, HEAD),
        P(None, SEQ, HEAD),
        P(None, HEAD, SEQ),
        P(SEQ, HEAD),
        P(HEAD, None, None),
        P(HEAD, None, None),
        P(HEAD, None, None),
        P(HEAD, None),
        P(None, SEQ),
    )

    def body(*args):
        return on_device(*args, ylen, zlen)

    return jax.shard_map(
        body, mesh=split, in_specs=in_specs, out_specs=P(SEQ, HEAD), check_vma=False
    )
```

```python
import jax
import jax.numpy as jnp
from jax import lax
from jax.experimental import pallas as pl
from jax.experimental.pallas import tpu as pltpu
from jax.sharding import Mesh
from jax.sharding import PartitionSpec as P


NS_ITERS = 3
GRADS_LIMIT = 52
PAIR_LIMIT = 44
HALF_LIMIT = 30
HEAD = ("z", "xh")
SEQ = ("xl", "y", "c")
CHIPS = ("xl", "y")


coef_a = 3.4445
coef_b = -4.775
coef_c = 2.0315
step_size = 0.5

BF = jnp.bfloat16
F32 = jnp.float32


def sds(shape, dtype):
    return jax.ShapeDtypeStruct(shape, dtype)


def vmem(count):
    return [pl.BlockSpec(memory_space=pltpu.VMEM)] * count


def smem():
    return pl.BlockSpec(memory_space=pltpu.SMEM)


def far_spec():
    return pl.BlockSpec(memory_space=pltpu.HBM)


def call(body, outs, in_specs, scratch=(), flops=0, limit=32):
    return pl.pallas_call(
        body,
        out_shape=outs,
        in_specs=in_specs,
        out_specs=jax.tree.map(lambda _: pl.BlockSpec(memory_space=pltpu.VMEM), outs),
        scratch_shapes=scratch,
        compiler_params=pltpu.CompilerParams(vmem_limit_bytes=limit << 20),
        cost_estimate=pl.CostEstimate(flops=flops, bytes_accessed=4 << 20, transcendentals=0),
    )


def dot(left, right):
    return jnp.dot(left, right, preferred_element_type=F32)


def dot_tn(left, right):
    return lax.dot_general(left, right, (((0,), (0,)), ((), ())), preferred_element_type=F32)


def dot_nt(left, right):
    return lax.dot_general(left, right, (((1,), (1,)), ((), ())), preferred_element_type=F32)


def core_is_first():
    return lax.axis_index("c") == 0


def grads_body(
    keys_h, values_h, rates, first_h, third_h, second_h,
    mine, other, half, half_other,
    keys, values, first, third, second, hidden_s, weighted_s, bm_s, bo_s, sems,
):
    core0 = core_is_first()
    groups, rows, wide = keys_h.shape
    copies = {}

    def fetch(name, source, target):
        copies[name] = pltpu.make_async_copy(source, target, sems.at[len(copies)])
        copies[name].start()

    fetch("first", first_h.at[0], first)
    fetch("k0", keys_h.at[0], keys.at[pl.ds(0, rows)])
    fetch("third", third_h.at[0], third)
    fetch("v0", values_h.at[0], values.at[pl.ds(0, rows)])
    fetch("second", second_h.at[0], second)
    for group in range(1, groups):
        fetch(f"k{group}", keys_h.at[group], keys.at[pl.ds(group * rows, rows)])
        fetch(f"v{group}", values_h.at[group], values.at[pl.ds(group * rows, rows)])

    def ready(*names):
        for name in names:
            if name in copies:
                copies.pop(name).wait()

    tile = 256
    lanes = 128
    for group in range(groups):
        for part in range(rows // tile):
            block = pl.ds(group * rows + part * tile, tile)
            ready("first", f"k{group}", "third")
            k = keys[block, :]
            first_pre = dot(k, first[...])
            third_pre = dot(k, third[...])
            ready(f"v{group}", "second")
            row = rates[group, :, pl.ds(part * tile, tile)]
            scale = jnp.broadcast_to(row, (lanes, tile)).T
            scale = jnp.concatenate([scale] * (wide // lanes), axis=1)
            weighted = (values[block, :].astype(F32) * scale).astype(BF)
            weighted_s[block, :] = weighted
            sig = 1.0 / (1.0 + jnp.exp(-first_pre))
            swish = first_pre * sig
            hidden_s[block, :] = (swish * third_pre).astype(BF)
            back = dot_nt(weighted, second[...])
            back_first = (back * third_pre * sig * (1.0 + first_pre * (1.0 - sig))).astype(BF)
            back_third = (back * swish).astype(BF)
            bm_s[block, :] = jnp.where(core0, back_first, back_third)
            bo_s[block, :] = jnp.where(core0, back_third, back_first)
    mine[...] = dot_tn(keys[...], bm_s[...]).astype(BF)
    other[...] = dot_tn(keys[...], bo_s[...]).astype(BF)
    low = wide // 2
    total = dot_tn(hidden_s[...], weighted_s[...])
    half[...] = jnp.where(core0, total[:low], total[low:]).astype(BF)
    half_other[...] = jnp.where(core0, total[low:], total[:low]).astype(BF)


def grads(keys, values, rates, first, third, second):
    groups, rows, wide = keys.shape
    total = groups * rows
    tokens = pltpu.VMEM((total, wide), BF)
    weight = pltpu.VMEM((wide, wide), BF)
    return call(
        grads_body,
        (
            sds((wide, wide), BF),
            sds((wide, wide), BF),
            sds((wide // 2, wide), BF),
            sds((wide // 2, wide), BF),
        ),
        [far_spec(), far_spec(), vmem(1)[0]] + [far_spec()] * 3,
        [tokens, tokens, weight, weight, weight]
        + [tokens] * 4
        + [pltpu.SemaphoreType.DMA((3 + 2 * groups,))],
        flops=6 * 2 * total * wide * wide,
        limit=GRADS_LIMIT,
    )(keys, values, rates, first, third, second)


def fold_body(mine, got, half, half_got, out):
    chips = out.shape[0]
    rows = mine.shape[0] // chips
    less = half.shape[0] // chips
    for index in range(chips):
        for own, more, base, size in ((mine, got, 0, rows), (half, half_got, rows, less)):
            span = pl.ds(index * size, size)
            total = own[span, :].astype(F32) + more[span, :].astype(F32)
            out[index, pl.ds(base, size), :] = total.astype(BF)


def fold(mine, got, half, half_got, chips):
    wide = mine.shape[1]
    out = sds((chips, (mine.shape[0] + half.shape[0]) // chips, wide), BF)
    return call(fold_body, out, vmem(4), flops=1 << 27, limit=10)(mine, got, half, half_got)


def spread_body(parts, pair, half):
    total = parts[0].astype(F32)
    for index in range(1, parts.shape[0]):
        total = total + parts[index].astype(F32)
    low = total.astype(BF)
    rows = pair.shape[1]
    for index in range(parts.shape[0]):
        pair[index] = low[:rows]
        half[index] = low[rows:]


def spread(parts, rows):
    chips, both, wide = parts.shape
    outs = (sds((chips, rows, wide), BF), sds((chips, both - rows, wide), BF))
    return call(spread_body, outs, vmem(1), flops=1 << 27, limit=10)(parts)


def trade(parts):
    return lax.all_to_all(parts, CHIPS, 0, 0)


def ns_core(full, x_s):
    grad = full[...]
    scale = jnp.sqrt(jnp.sum(grad * grad)) + 1e-06
    x_s[...] = (grad / scale).astype(BF)

    def step(_, carry):
        x = x_s[...]
        gram = dot_nt(x, x)
        low = gram.astype(BF)
        poly = (coef_b * gram + coef_c * dot(low, low)).astype(BF)
        x_s[...] = (coef_a * x.astype(F32) + dot(poly, x)).astype(BF)
        return carry

    lax.fori_loop(0, NS_ITERS, step, 0)


def renew(old, x_s, out):
    fresh = old + step_size * x_s[...].astype(F32)
    ratio = jnp.sqrt(jnp.mean(old * old, axis=0, keepdims=True) + 1e-06) / jnp.sqrt(
        jnp.mean(fresh * fresh, axis=0, keepdims=True) + 1e-06
    )
    out[...] = (fresh * ratio).astype(BF)


def begin(copies, sems):
    started = [
        pltpu.make_async_copy(source, target, sems.at[index])
        for index, (source, target) in enumerate(copies)
    ]
    for copy in started:
        copy.start()
    return started


def ns_pair_body(places, zlen, totals, first, third, weight_h, queries_h, out, queries, *refs):
    count = len(places)
    blocks, (full, x_s, sems) = refs[:count], refs[count:]
    z = lax.axis_index("z")
    x = lax.axis_index("xh")
    wide = out.shape[1]
    columns = [lax.rem(z + dz, zlen) * 2 + lax.rem(x + dx, 2) for dz, dx in places]
    copies = begin(
        [(queries_h, queries)]
        + [
            (weight_h.at[:, pl.ds(pl.multiple_of(column * wide, 128), wide)], block)
            for column, block in zip(columns, blocks)
        ],
        sems,
    )
    chips = totals.shape[0]
    rows = full.shape[0] // chips
    for index in range(chips):
        full[pl.ds(index * rows, rows), :] = totals[index].astype(F32)
    ns_core(full, x_s)
    old = jnp.where(core_is_first(), first[...], third[...]).astype(F32)
    renew(old, x_s, out)
    for copy in copies:
        copy.wait()


def ns_half_body(own, got, second, out, full, x_s):
    core0 = core_is_first()
    chips, rows, _ = own.shape
    low = chips * rows
    for index in range(chips):
        a = own[index].astype(F32)
        b = got[index].astype(F32)
        full[pl.ds(index * rows, rows), :] = jnp.where(core0, a, b)
        full[pl.ds(low + index * rows, rows), :] = jnp.where(core0, b, a)
    ns_core(full, x_s)
    renew(second[...].astype(F32), x_s, out)


def ns_scratch(wide):
    return [pltpu.VMEM((wide, wide), F32), pltpu.VMEM((wide, wide), BF)]


def ns_pair(places, zlen, totals, first, third, out_weight, queries):
    wide = first.shape[1]
    weight = sds((wide, wide), BF)

    def body(*refs):
        ns_pair_body(places, zlen, *refs)

    return call(
        body,
        (weight, sds(queries.shape, BF)) + (weight,) * len(places),
        vmem(3) + [far_spec()] * 2,
        ns_scratch(wide) + [pltpu.SemaphoreType.DMA((1 + len(places),))],
        flops=9 * 2 * wide**3,
        limit=PAIR_LIMIT,
    )(totals, first, third, out_weight, queries)


def ns_half(own, got, second):
    wide = second.shape[1]
    return call(
        ns_half_body,
        sds((wide, wide), BF),
        vmem(3),
        ns_scratch(wide),
        flops=9 * 2 * wide**3,
        limit=HALF_LIMIT,
    )(own, got, second)


def apply_body(counts, queries, mine, got, second, far, out, far_top, far_low):
    core0 = core_is_first()
    rows, wide = out.shape
    limit = counts[0, counts.shape[1] - 1]
    tile = rows // 2
    for part, far_out in enumerate((far_top, far_low)):
        span = pl.ds(part * tile, tile)
        q = queries[span, :]
        a = dot(q, mine[...])
        b = dot(q, got[...])
        first_pre = jnp.where(core0, a, b)
        third_pre = jnp.where(core0, b, a)
        hidden = (first_pre / (1.0 + jnp.exp(-first_pre)) * third_pre).astype(BF)
        spot = lax.broadcasted_iota(jnp.int32, (tile, wide), 0) + part * tile
        head = jnp.where(spot < limit, dot(hidden, second[...]), 0.0).astype(BF)
        out[span, :] = head
        far_out[...] = dot(head, far[...]).astype(BF)


def cross_body(x, same, up, down, cross, same_top, same_low, hold_up, hold_down):
    half = same_top.shape[0]
    top, low = pl.ds(0, half), pl.ds(half, half)
    cross[top, :] = dot(x[top, :], down[...]).astype(BF)
    cross[low, :] = dot(x[low, :], up[...]).astype(BF)
    same_top[...] = dot(x[top, :], same[...]).astype(BF)
    same_low[...] = dot(x[low, :], same[...]).astype(BF)
    hold_up[...] = dot(x[top, :], up[...])
    hold_down[...] = dot(x[low, :], down[...])


def project_body(x, after, *refs):
    count = len(refs) // 2
    for block, out in zip(refs[:count], refs[count:]):
        out[...] = dot(x[...], block[...])


def turn(count, by):
    return [(index, (index + by) % count) for index in range(count)]


PLACES = ((2, 1), (2, 0), (1, 1), (3, 1), (1, 0), (3, 0), (0, 1), (0, 0))


def mixed_sum(counts, queries, new_mine, new_got, new_second, blocks, zlen):
    rows, cols = queries.shape
    half = rows // 2
    one = 2 * rows * cols * cols

    def send(value, axis, by):
        return lax.ppermute(value, axis, turn({"z": zlen, "xh": 2}[axis], by))

    def wide(*values):
        return sum(value.astype(F32) for value in values)

    full, part = (rows, cols), (half, cols)
    head_out, far_top, far_low = call(
        apply_body,
        (sds(full, BF), sds(part, BF), sds(part, BF)),
        [smem()] + vmem(5),
        flops=4 * one,
        limit=24,
    )(counts, queries, new_mine, new_got, new_second, blocks[0])
    far_top = send(far_top, "z", 1)
    far_low = send(far_low, "z", zlen - 1)
    cross, same_top, same_low, hold_up, hold_down = call(
        cross_body,
        (sds(full, BF), sds(part, BF), sds(part, BF), sds(part, F32), sds(part, F32)),
        vmem(4),
        flops=3 * one,
        limit=24,
    )(head_out, *blocks[1:4])
    cross = send(cross, "xh", 1)
    same_top = send(same_top, "z", 1)
    same_low = send(same_low, "z", zlen - 1)
    next_up, next_down, next_over, own = call(
        project_body, (sds(full, F32),) * 4, vmem(1) + [pl.BlockSpec(memory_space=pl.ANY)] + vmem(4),
        flops=4 * one, limit=24,
    )(head_out, hold_up, *blocks[4:])
    by_up = send(wide(hold_up, far_top).astype(BF), "z", 1)
    by_down = send(wide(hold_down, far_low).astype(BF), "z", zlen - 1)
    to_up = wide(next_up, jnp.concatenate([same_top, cross[half:]])).astype(BF)
    to_down = wide(next_down, jnp.concatenate([cross[:half], same_low])).astype(BF)
    from_low = send(to_up, "z", 1)
    from_high = send(to_down, "z", zlen - 1)
    over_top = send(add_rows(next_over, by_up, 0), "xh", 1)
    over_low = send(add_rows(next_over, by_down, half), "xh", 1)
    from_over = jnp.concatenate([over_top, over_low])
    return wide(own, from_low, from_high, from_over).astype(BF)


def add_rows(full, more, start):
    rows = more.shape[0]

    def body(a, b, out):
        out[...] = (a[pl.ds(start, rows), :] + b[...].astype(F32)).astype(BF)

    return call(body, sds(more.shape, BF), vmem(2), flops=1 << 24, limit=8)(full, more)


def on_device(
    keys, values, step_rates, queries, first_weight, third_weight, second_weight, out_weight,
    live_counts, ylen, zlen,
):
    first, third = first_weight[0], third_weight[0]
    swap = lambda v: lax.ppermute(v, "c", turn(2, 1))

    counts = live_counts.T
    groups, rows, _ = keys.shape
    live = jnp.arange(rows, dtype=jnp.int32)[None, None, :] < live_counts[:groups, :, None]
    scales = jnp.where(live, step_rates, 0.0)
    mine, other, half, half_other = grads(
        keys, values, scales, first_weight, third_weight, second_weight
    )
    folded = fold(mine, swap(other), half, swap(half_other), 2 * ylen)
    pair, halves = spread(trade(folded), mine.shape[0] // (2 * ylen))
    halves = trade(halves)
    halves_got = swap(halves)
    pair = trade(pair)
    new_second = ns_half(halves, halves_got, second_weight[0])
    new_mine, near_queries, *blocks = ns_pair(PLACES, zlen, pair, first, third, out_weight, queries)
    new_got = swap(new_mine)
    return mixed_sum(counts, near_queries, new_mine, new_got, new_second, blocks, zlen)


def solution(mesh):
    xlen, ylen, zlen = 2, 4, 4
    split = Mesh(mesh.devices.reshape(zlen, 2, xlen, ylen, 2), HEAD + SEQ)
    in_specs = (
        P(None, SEQ, HEAD),
        P(None, SEQ, HEAD),
        P(None, HEAD, SEQ),
        P(SEQ, HEAD),
        P(HEAD, None, None),
        P(HEAD, None, None),
        P(HEAD, None, None),
        P(HEAD, None),
        P(None, SEQ),
    )

    def body(*args):
        return on_device(*args, ylen, zlen)

    return jax.shard_map(
        body, mesh=split, in_specs=in_specs, out_specs=P(SEQ, HEAD), check_vma=False
    )
```

```python
import jax
import jax.numpy as jnp
from jax import lax
from jax.experimental import pallas as pl
from jax.experimental.pallas import tpu as pltpu
from jax.sharding import Mesh
from jax.sharding import PartitionSpec as P


NS_ITERS = 3
GRADS_LIMIT = 52
PAIR_LIMIT = 30
HALF_LIMIT = 40
HEAD = ("z", "xh")
SEQ = ("xl", "y", "c")
CHIPS = ("xl", "y")


coef_a = 3.4445
coef_b = -4.775
coef_c = 2.0315
step_size = 0.5

BF = jnp.bfloat16
F32 = jnp.float32


def sds(shape, dtype):
    return jax.ShapeDtypeStruct(shape, dtype)


def vmem(count):
    return [pl.BlockSpec(memory_space=pltpu.VMEM)] * count


def smem():
    return pl.BlockSpec(memory_space=pltpu.SMEM)


def far_spec():
    return pl.BlockSpec(memory_space=pltpu.HBM)


def call(body, outs, in_specs, scratch=(), flops=0, limit=32):
    return pl.pallas_call(
        body,
        out_shape=outs,
        in_specs=in_specs,
        out_specs=jax.tree.map(lambda _: pl.BlockSpec(memory_space=pltpu.VMEM), outs),
        scratch_shapes=scratch,
        compiler_params=pltpu.CompilerParams(vmem_limit_bytes=limit << 20),
        cost_estimate=pl.CostEstimate(flops=flops, bytes_accessed=4 << 20, transcendentals=0),
    )


def dot(left, right):
    return jnp.dot(left, right, preferred_element_type=F32)


def dot_tn(left, right):
    return lax.dot_general(left, right, (((0,), (0,)), ((), ())), preferred_element_type=F32)


def dot_nt(left, right):
    return lax.dot_general(left, right, (((1,), (1,)), ((), ())), preferred_element_type=F32)


def core_is_first():
    return lax.axis_index("c") == 0


def grads_body(
    keys_h, values_h, rates, first_h, third_h, second_h,
    mine, other, half, half_other,
    keys, values, first, third, second, hidden_s, weighted_s, bm_s, bo_s, sems,
):
    core0 = core_is_first()
    groups, rows, wide = keys_h.shape
    copies = {}

    def fetch(name, source, target):
        copies[name] = pltpu.make_async_copy(source, target, sems.at[len(copies)])
        copies[name].start()

    fetch("first", first_h.at[0], first)
    fetch("k0", keys_h.at[0], keys.at[pl.ds(0, rows)])
    fetch("third", third_h.at[0], third)
    fetch("v0", values_h.at[0], values.at[pl.ds(0, rows)])
    fetch("second", second_h.at[0], second)
    for group in range(1, groups):
        fetch(f"k{group}", keys_h.at[group], keys.at[pl.ds(group * rows, rows)])
        fetch(f"v{group}", values_h.at[group], values.at[pl.ds(group * rows, rows)])

    def ready(*names):
        for name in names:
            if name in copies:
                copies.pop(name).wait()

    tile = 256
    lanes = 128
    for group in range(groups):
        for part in range(rows // tile):
            block = pl.ds(group * rows + part * tile, tile)
            ready("first", f"k{group}", "third")
            k = keys[block, :]
            first_pre = dot(k, first[...])
            third_pre = dot(k, third[...])
            ready(f"v{group}", "second")
            row = rates[group, :, pl.ds(part * tile, tile)]
            scale = jnp.broadcast_to(row, (lanes, tile)).T
            scale = jnp.concatenate([scale] * (wide // lanes), axis=1)
            weighted = (values[block, :].astype(F32) * scale).astype(BF)
            weighted_s[block, :] = weighted
            sig = 1.0 / (1.0 + jnp.exp(-first_pre))
            swish = first_pre * sig
            hidden_s[block, :] = (swish * third_pre).astype(BF)
            back = dot_nt(weighted, second[...])
            back_first = (back * third_pre * sig * (1.0 + first_pre * (1.0 - sig))).astype(BF)
            back_third = (back * swish).astype(BF)
            bm_s[block, :] = jnp.where(core0, back_first, back_third)
            bo_s[block, :] = jnp.where(core0, back_third, back_first)
    mine[...] = dot_tn(keys[...], bm_s[...]).astype(BF)
    other[...] = dot_tn(keys[...], bo_s[...]).astype(BF)
    low = wide // 2
    total = dot_tn(hidden_s[...], weighted_s[...])
    half[...] = jnp.where(core0, total[:low], total[low:]).astype(BF)
    half_other[...] = jnp.where(core0, total[low:], total[:low]).astype(BF)


def grads(keys, values, rates, first, third, second):
    groups, rows, wide = keys.shape
    total = groups * rows
    tokens = pltpu.VMEM((total, wide), BF)
    weight = pltpu.VMEM((wide, wide), BF)
    return call(
        grads_body,
        (
            sds((wide, wide), BF),
            sds((wide, wide), BF),
            sds((wide // 2, wide), BF),
            sds((wide // 2, wide), BF),
        ),
        [far_spec(), far_spec(), vmem(1)[0]] + [far_spec()] * 3,
        [tokens, tokens, weight, weight, weight]
        + [tokens] * 4
        + [pltpu.SemaphoreType.DMA((3 + 2 * groups,))],
        flops=6 * 2 * total * wide * wide,
        limit=GRADS_LIMIT,
    )(keys, values, rates, first, third, second)


def fold_body(mine, got, half, half_got, out):
    chips = out.shape[0]
    rows = mine.shape[0] // chips
    less = half.shape[0] // chips
    for index in range(chips):
        for own, more, base, size in ((mine, got, 0, rows), (half, half_got, rows, less)):
            span = pl.ds(index * size, size)
            total = own[span, :].astype(F32) + more[span, :].astype(F32)
            out[index, pl.ds(base, size), :] = total.astype(BF)


def fold(mine, got, half, half_got, chips):
    wide = mine.shape[1]
    out = sds((chips, (mine.shape[0] + half.shape[0]) // chips, wide), BF)
    return call(fold_body, out, vmem(4), flops=1 << 27, limit=10)(mine, got, half, half_got)


def spread_body(parts, out):
    total = parts[0].astype(F32)
    for index in range(1, parts.shape[0]):
        total = total + parts[index].astype(F32)
    for index in range(parts.shape[0]):
        out[index] = total.astype(BF)


def spread(parts):
    return call(spread_body, sds(parts.shape, BF), vmem(1), flops=1 << 27, limit=10)(parts)


def trade(parts):
    return lax.all_to_all(parts, CHIPS, 0, 0)


def column_spans(wide):
    return [(start, min(256, wide - start)) for start in range(0, wide, 256)]


def store_symmetric(target, lower, start, size):
    target[start:, start : start + size] = lower
    if start + size < target.shape[0]:
        target[start : start + size, start + size :] = lower[size:, :].T


def poly_step(x, out, gram_s, low_s, poly_s):
    wide = x.shape[0]
    for start, size in column_spans(wide):
        gram = dot_nt(x[start:, :], x[start : start + size, :])
        gram_s[start:, start : start + size] = gram
        store_symmetric(low_s, gram.astype(BF), start, size)
    for start, size in column_spans(wide):
        square = dot(low_s[start:, :], low_s[:, start : start + size])
        poly = coef_b * gram_s[start:, start : start + size] + coef_c * square
        store_symmetric(poly_s, poly.astype(BF), start, size)
    for start, size in column_spans(wide):
        span = slice(start, start + size)
        out[:, span] = (coef_a * x[:, span].astype(F32) + dot(poly_s[...], x[:, span])).astype(BF)


def ns_core(full, x_a, x_b, *scratch):
    grad = full[...]
    scale = jnp.sqrt(jnp.sum(grad * grad)) + 1e-06
    x_a[...] = (full[...] * (1.0 / scale)).astype(BF)
    for _ in range(NS_ITERS):
        poly_step(x_a, x_b, *scratch)
        x_a, x_b = x_b, x_a
    return x_a


def renew(old, x_s, out):
    fresh = old + step_size * x_s[...].astype(F32)
    ratio = jnp.sqrt(jnp.mean(old * old, axis=0, keepdims=True) + 1e-06) / jnp.sqrt(
        jnp.mean(fresh * fresh, axis=0, keepdims=True) + 1e-06
    )
    out[...] = (fresh * ratio).astype(BF)


def begin(copies, sems):
    started = [
        pltpu.make_async_copy(source, target, sems.at[index])
        for index, (source, target) in enumerate(copies)
    ]
    for copy in started:
        copy.start()
    return started


def ns_pair_body(totals, first, third, second_h, queries_h, out, second, queries, full, *rest):
    work, sems = rest[:-1], rest[-1]
    copies = begin([(second_h.at[0], second), (queries_h, queries)], sems)
    chips = totals.shape[0]
    rows = full.shape[0] // chips
    for index in range(chips):
        full[pl.ds(index * rows, rows), :] = totals[index, pl.ds(0, rows), :].astype(F32)
    old = jnp.where(core_is_first(), first[...], third[...]).astype(F32)
    renew(old, ns_core(full, *work), out)
    for copy in copies:
        copy.wait()


def ns_half_body(places, zlen, own, got, second, weight_h, out, *refs):
    count = len(places)
    blocks, full, work, sems = refs[:count], refs[count], refs[count + 1 : -1], refs[-1]
    z = lax.axis_index("z")
    x = lax.axis_index("xh")
    wide = out.shape[1]
    columns = [lax.rem(z + dz, zlen) * 2 + lax.rem(x + dx, 2) for dz, dx in places]
    copies = begin(
        [
            (weight_h.at[:, pl.ds(pl.multiple_of(column * wide, 128), wide)], block)
            for column, block in zip(columns, blocks)
        ],
        sems,
    )
    core0 = core_is_first()
    chips = own.shape[0]
    low = wide // 2
    rows = low // chips
    part = pl.ds(own.shape[1] - rows, rows)
    for index in range(chips):
        a = own[index, part, :].astype(F32)
        b = got[index, part, :].astype(F32)
        full[pl.ds(index * rows, rows), :] = jnp.where(core0, a, b)
        full[pl.ds(low + index * rows, rows), :] = jnp.where(core0, b, a)
    renew(second[...].astype(F32), ns_core(full, *work), out)
    for copy in copies:
        copy.wait()


def ns_scratch(wide, copies):
    return [
        pltpu.VMEM((wide, wide), F32),
        pltpu.VMEM((wide, wide), BF),
        pltpu.VMEM((wide, wide), BF),
        pltpu.VMEM((wide, wide), F32),
        pltpu.VMEM((wide, wide), BF),
        pltpu.VMEM((wide, wide), BF),
        pltpu.SemaphoreType.DMA((copies,)),
    ]


def ns_pair(totals, first, third, second, queries):
    wide = first.shape[1]
    weight = sds((wide, wide), BF)
    return call(
        ns_pair_body,
        (weight, weight, sds(queries.shape, BF)),
        vmem(3) + [far_spec()] * 2,
        ns_scratch(wide, 2),
        flops=9 * 2 * wide**3,
        limit=PAIR_LIMIT,
    )(totals, first, third, second, queries)


def ns_half(places, zlen, own, got, second, out_weight):
    wide = second.shape[1]

    def body(*refs):
        ns_half_body(places, zlen, *refs)

    return call(
        body,
        (sds((wide, wide), BF),) * (1 + len(places)),
        vmem(3) + [far_spec()],
        ns_scratch(wide, len(places)),
        flops=9 * 2 * wide**3,
        limit=HALF_LIMIT,
    )(own, got, second, out_weight)


def apply_body(counts, queries, mine, got, second, far, out, far_top, far_low):
    core0 = core_is_first()
    rows, wide = out.shape
    limit = counts[0, counts.shape[1] - 1]
    tile = rows // 2
    for part, far_out in enumerate((far_top, far_low)):
        span = pl.ds(part * tile, tile)
        q = queries[span, :]
        a = dot(q, mine[...])
        b = dot(q, got[...])
        first_pre = jnp.where(core0, a, b)
        third_pre = jnp.where(core0, b, a)
        hidden = (first_pre / (1.0 + jnp.exp(-first_pre)) * third_pre).astype(BF)
        spot = lax.broadcasted_iota(jnp.int32, (tile, wide), 0) + part * tile
        head = jnp.where(spot < limit, dot(hidden, second[...]), 0.0).astype(BF)
        out[span, :] = head
        far_out[...] = dot(head, far[...]).astype(BF)


def cross_body(x, same, up, down, cross, same_top, same_low, hold_up, hold_down):
    half = same_top.shape[0]
    top, low = pl.ds(0, half), pl.ds(half, half)
    cross[top, :] = dot(x[top, :], down[...]).astype(BF)
    cross[low, :] = dot(x[low, :], up[...]).astype(BF)
    same_top[...] = dot(x[top, :], same[...]).astype(BF)
    same_low[...] = dot(x[low, :], same[...]).astype(BF)
    hold_up[...] = dot(x[top, :], up[...])
    hold_down[...] = dot(x[low, :], down[...])


def project_body(x, after, *refs):
    count = len(refs) // 2
    for block, out in zip(refs[:count], refs[count:]):
        out[...] = dot(x[...], block[...])


def turn(count, by):
    return [(index, (index + by) % count) for index in range(count)]


PLACES = ((2, 1), (2, 0), (1, 1), (3, 1), (1, 0), (3, 0), (0, 1), (0, 0))


def mixed_sum(counts, queries, new_mine, new_got, new_second, blocks, zlen):
    rows, cols = queries.shape
    half = rows // 2
    one = 2 * rows * cols * cols

    def send(value, axis, by):
        return lax.ppermute(value, axis, turn({"z": zlen, "xh": 2}[axis], by))

    def wide(*values):
        return sum(value.astype(F32) for value in values)

    full, part = (rows, cols), (half, cols)
    head_out, far_top, far_low = call(
        apply_body,
        (sds(full, BF), sds(part, BF), sds(part, BF)),
        [smem()] + vmem(5),
        flops=4 * one,
        limit=24,
    )(counts, queries, new_mine, new_got, new_second, blocks[0])
    far_top = send(far_top, "z", 1)
    far_low = send(far_low, "z", zlen - 1)
    cross, same_top, same_low, hold_up, hold_down = call(
        cross_body,
        (sds(full, BF), sds(part, BF), sds(part, BF), sds(part, F32), sds(part, F32)),
        vmem(4),
        flops=3 * one,
        limit=24,
    )(head_out, *blocks[1:4])
    cross = send(cross, "xh", 1)
    same_top = send(same_top, "z", 1)
    same_low = send(same_low, "z", zlen - 1)
    next_up, next_down, next_over, own = call(
        project_body, (sds(full, F32),) * 4, vmem(1) + [pl.BlockSpec(memory_space=pl.ANY)] + vmem(4),
        flops=4 * one, limit=24,
    )(head_out, hold_up, *blocks[4:])
    by_up = send(wide(hold_up, far_top).astype(BF), "z", 1)
    by_down = send(wide(hold_down, far_low).astype(BF), "z", zlen - 1)
    to_up = wide(next_up, jnp.concatenate([same_top, cross[half:]])).astype(BF)
    to_down = wide(next_down, jnp.concatenate([cross[:half], same_low])).astype(BF)
    from_low = send(to_up, "z", 1)
    from_high = send(to_down, "z", zlen - 1)
    over_top = send(add_rows(next_over, by_up, 0), "xh", 1)
    over_low = send(add_rows(next_over, by_down, half), "xh", 1)
    from_over = jnp.concatenate([over_top, over_low])
    return wide(own, from_low, from_high, from_over).astype(BF)


def add_rows(full, more, start):
    rows = more.shape[0]

    def body(a, b, out):
        out[...] = (a[pl.ds(start, rows), :] + b[...].astype(F32)).astype(BF)

    return call(body, sds(more.shape, BF), vmem(2), flops=1 << 24, limit=8)(full, more)


def on_device(
    keys, values, step_rates, queries, first_weight, third_weight, second_weight, out_weight,
    live_counts, ylen, zlen,
):
    first, third = first_weight[0], third_weight[0]
    swap = lambda v: lax.ppermute(v, "c", turn(2, 1))

    counts = live_counts.T
    groups, rows, _ = keys.shape
    live = jnp.arange(rows, dtype=jnp.int32)[None, None, :] < live_counts[:groups, :, None]
    scales = jnp.where(live, step_rates, 0.0)
    mine, other, half, half_other = grads(
        keys, values, scales, first_weight, third_weight, second_weight
    )
    totals = trade(spread(trade(fold(mine, swap(other), half, swap(half_other), 2 * ylen))))
    totals_got = swap(totals)
    new_mine, second, near_queries = ns_pair(totals, first, third, second_weight, queries)
    new_got = swap(new_mine)
    new_second, *blocks = ns_half(PLACES, zlen, totals, totals_got, second, out_weight)
    return mixed_sum(counts, near_queries, new_mine, new_got, new_second, blocks, zlen)


def solution(mesh):
    xlen, ylen, zlen = 2, 4, 4
    split = Mesh(mesh.devices.reshape(zlen, 2, xlen, ylen, 2), HEAD + SEQ)
    in_specs = (
        P(None, SEQ, HEAD),
        P(None, SEQ, HEAD),
        P(None, HEAD, SEQ),
        P(SEQ, HEAD),
        P(HEAD, None, None),
        P(HEAD, None, None),
        P(HEAD, None, None),
        P(HEAD, None),
        P(None, SEQ),
    )

    def body(*args):
        return on_device(*args, ylen, zlen)

    return jax.shard_map(
        body, mesh=split, in_specs=in_specs, out_specs=P(SEQ, HEAD), check_vma=False
    )
```

```python
import functools

import jax
import jax.numpy as jnp
from jax import lax
from jax.experimental import pallas as pl
from jax.experimental.pallas import tpu as pltpu
from jax.sharding import Mesh
from jax.sharding import PartitionSpec as P


NS_ITERS = 3
GRADS_LIMIT = 52
PAIR_LIMIT = 30
HALF_LIMIT = 30
HEAD = ("z", "xh")
SEQ = ("xl", "y", "c")
CHIPS = ("xl", "y")


coef_a = 3.4445
coef_b = -4.775
coef_c = 2.0315
step_size = 0.5

BF = jnp.bfloat16
F32 = jnp.float32


def sds(shape, dtype):
    return jax.ShapeDtypeStruct(shape, dtype)


def vmem(count):
    return [pl.BlockSpec(memory_space=pltpu.VMEM)] * count


def smem():
    return pl.BlockSpec(memory_space=pltpu.SMEM)


def far_spec():
    return pl.BlockSpec(memory_space=pltpu.HBM)


def call(body, outs, in_specs, scratch=(), flops=0, limit=32):
    return pl.pallas_call(
        body,
        out_shape=outs,
        in_specs=in_specs,
        out_specs=jax.tree.map(lambda _: pl.BlockSpec(memory_space=pltpu.VMEM), outs),
        scratch_shapes=scratch,
        compiler_params=pltpu.CompilerParams(vmem_limit_bytes=limit << 20),
        cost_estimate=pl.CostEstimate(flops=flops, bytes_accessed=4 << 20, transcendentals=0),
    )


def dot(left, right):
    return jnp.dot(left, right, preferred_element_type=F32)


def dot_tn(left, right):
    return lax.dot_general(left, right, (((0,), (0,)), ((), ())), preferred_element_type=F32)


def dot_nt(left, right):
    return lax.dot_general(left, right, (((1,), (1,)), ((), ())), preferred_element_type=F32)


def core_is_first():
    return lax.axis_index("c") == 0


def grads_body(
    keys_h, values_h, rates, first_h, third_h, second_h,
    mine, other, half, half_other,
    keys, values, first, third, second, hidden_s, weighted_s, bm_s, bo_s, sems,
):
    core0 = core_is_first()
    groups, rows, wide = keys_h.shape
    copies = {}

    def fetch(name, source, target):
        copies[name] = pltpu.make_async_copy(source, target, sems.at[len(copies)])
        copies[name].start()

    fetch("first", first_h.at[0], first)
    fetch("k0", keys_h.at[0], keys.at[pl.ds(0, rows)])
    fetch("third", third_h.at[0], third)
    fetch("v0", values_h.at[0], values.at[pl.ds(0, rows)])
    fetch("second", second_h.at[0], second)
    for group in range(1, groups):
        fetch(f"k{group}", keys_h.at[group], keys.at[pl.ds(group * rows, rows)])
        fetch(f"v{group}", values_h.at[group], values.at[pl.ds(group * rows, rows)])

    def ready(*names):
        for name in names:
            if name in copies:
                copies.pop(name).wait()

    tile = 256
    lanes = 128
    for group in range(groups):
        for part in range(rows // tile):
            block = pl.ds(group * rows + part * tile, tile)
            ready("first", f"k{group}", "third")
            k = keys[block, :]
            first_pre = dot(k, first[...])
            third_pre = dot(k, third[...])
            ready(f"v{group}", "second")
            row = rates[group, :, pl.ds(part * tile, tile)]
            scale = jnp.broadcast_to(row, (lanes, tile)).T
            scale = jnp.concatenate([scale] * (wide // lanes), axis=1)
            weighted = (values[block, :].astype(F32) * scale).astype(BF)
            weighted_s[block, :] = weighted
            sig = 1.0 / (1.0 + jnp.exp(-first_pre))
            swish = first_pre * sig
            hidden_s[block, :] = (swish * third_pre).astype(BF)
            back = dot_nt(weighted, second[...])
            back_first = (back * third_pre * sig * (1.0 + first_pre * (1.0 - sig))).astype(BF)
            back_third = (back * swish).astype(BF)
            bm_s[block, :] = jnp.where(core0, back_first, back_third)
            bo_s[block, :] = jnp.where(core0, back_third, back_first)
    mine[...] = dot_tn(keys[...], bm_s[...]).astype(BF)
    other[...] = dot_tn(keys[...], bo_s[...]).astype(BF)
    low = wide // 2
    total = dot_tn(hidden_s[...], weighted_s[...])
    half[...] = jnp.where(core0, total[:low], total[low:]).astype(BF)
    half_other[...] = jnp.where(core0, total[low:], total[:low]).astype(BF)


def grads(keys, values, rates, first, third, second):
    groups, rows, wide = keys.shape
    total = groups * rows
    tokens = pltpu.VMEM((total, wide), BF)
    weight = pltpu.VMEM((wide, wide), BF)
    return call(
        grads_body,
        (
            sds((wide, wide), BF),
            sds((wide, wide), BF),
            sds((wide // 2, wide), BF),
            sds((wide // 2, wide), BF),
        ),
        [far_spec(), far_spec(), vmem(1)[0]] + [far_spec()] * 3,
        [tokens, tokens, weight, weight, weight]
        + [tokens] * 4
        + [pltpu.SemaphoreType.DMA((3 + 2 * groups,))],
        flops=6 * 2 * total * wide * wide,
        limit=GRADS_LIMIT,
    )(keys, values, rates, first, third, second)


def fold_body(mine, got, half, half_got, out):
    chips = out.shape[0]
    rows = mine.shape[0] // chips
    less = half.shape[0] // chips
    for index in range(chips):
        for own, more, base, size in ((mine, got, 0, rows), (half, half_got, rows, less)):
            span = pl.ds(index * size, size)
            total = own[span, :].astype(F32) + more[span, :].astype(F32)
            out[index, pl.ds(base, size), :] = total.astype(BF)


def fold(mine, got, half, half_got, chips):
    wide = mine.shape[1]
    out = sds((chips, (mine.shape[0] + half.shape[0]) // chips, wide), BF)
    return call(fold_body, out, vmem(4), flops=1 << 27, limit=10)(mine, got, half, half_got)


def spread_body(parts, out):
    total = parts[0].astype(F32)
    for index in range(1, parts.shape[0]):
        total = total + parts[index].astype(F32)
    for index in range(parts.shape[0]):
        out[index] = total.astype(BF)


def spread(parts):
    return call(spread_body, sds(parts.shape, BF), vmem(1), flops=1 << 27, limit=10)(parts)


def trade(parts):
    return lax.all_to_all(parts, CHIPS, 0, 0)


def column_spans(wide):
    return [(start, min(256, wide - start)) for start in range(0, wide, 256)]


def store_symmetric(target, lower, start, size):
    target[start:, start : start + size] = lower
    if start + size < target.shape[0]:
        target[start : start + size, start + size :] = lower[size:, :].T


def poly_step(x, out, gram_s, low_s, poly_s):
    wide = x.shape[0]
    for start, size in column_spans(wide):
        gram = dot_nt(x[start:, :], x[start : start + size, :])
        gram_s[start:, start : start + size] = gram
        store_symmetric(low_s, gram.astype(BF), start, size)
    for start, size in column_spans(wide):
        square = dot(low_s[start:, :], low_s[:, start : start + size])
        poly = coef_b * gram_s[start:, start : start + size] + coef_c * square
        store_symmetric(poly_s, poly.astype(BF), start, size)
    for start, size in column_spans(wide):
        span = slice(start, start + size)
        out[:, span] = (coef_a * x[:, span].astype(F32) + dot(poly_s[...], x[:, span])).astype(BF)


def ns_core(full, x_a, x_b, *scratch):
    grad = full[...]
    scale = jnp.sqrt(jnp.sum(grad * grad)) + 1e-06
    x_a[...] = (full[...] * (1.0 / scale)).astype(BF)
    for _ in range(NS_ITERS):
        poly_step(x_a, x_b, *scratch)
        x_a, x_b = x_b, x_a
    return x_a


def renew(old, x_s, out):
    fresh = old + step_size * x_s[...].astype(F32)
    ratio = jnp.sqrt(jnp.mean(old * old, axis=0, keepdims=True) + 1e-06) / jnp.sqrt(
        jnp.mean(fresh * fresh, axis=0, keepdims=True) + 1e-06
    )
    out[...] = (fresh * ratio).astype(BF)


def begin(copies, sems):
    started = [
        pltpu.make_async_copy(source, target, sems.at[index])
        for index, (source, target) in enumerate(copies)
    ]
    for copy in started:
        copy.start()
    return started


def ns_pair_body(totals, first, third, second_h, queries_h, out, second, queries, full, *rest):
    work, sems = rest[:-1], rest[-1]
    copies = begin([(second_h.at[0], second), (queries_h, queries)], sems)
    chips = totals.shape[0]
    rows = full.shape[0] // chips
    for index in range(chips):
        full[pl.ds(index * rows, rows), :] = totals[index, pl.ds(0, rows), :].astype(F32)
    old = jnp.where(core_is_first(), first[...], third[...]).astype(F32)
    renew(old, ns_core(full, *work), out)
    for copy in copies:
        copy.wait()


def ns_half_body(own, got, second, _, out, full, *rest):
    work = rest[:-1]
    wide = out.shape[1]
    core0 = core_is_first()
    chips = own.shape[0]
    low = wide // 2
    rows = low // chips
    part = pl.ds(own.shape[1] - rows, rows)
    for index in range(chips):
        a = own[index, part, :].astype(F32)
        b = got[index, part, :].astype(F32)
        full[pl.ds(index * rows, rows), :] = jnp.where(core0, a, b)
        full[pl.ds(low + index * rows, rows), :] = jnp.where(core0, b, a)
    renew(second[...].astype(F32), ns_core(full, *work), out)


def ns_scratch(wide, copies):
    return [
        pltpu.VMEM((wide, wide), F32),
        pltpu.VMEM((wide, wide), BF),
        pltpu.VMEM((wide, wide), BF),
        pltpu.VMEM((wide, wide), F32),
        pltpu.VMEM((wide, wide), BF),
        pltpu.VMEM((wide, wide), BF),
        pltpu.SemaphoreType.DMA((copies,)),
    ]


def ns_pair(totals, first, third, second, queries):
    wide = first.shape[1]
    weight = sds((wide, wide), BF)
    return call(
        ns_pair_body,
        (weight, weight, sds(queries.shape, BF)),
        vmem(3) + [far_spec()] * 2,
        ns_scratch(wide, 2),
        flops=9 * 2 * wide**3,
        limit=PAIR_LIMIT,
    )(totals, first, third, second, queries)


def ns_half(own, got, second, out_weight):
    wide = second.shape[1]
    return call(
        ns_half_body,
        sds((wide, wide), BF),
        vmem(4),
        ns_scratch(wide, 1),
        flops=9 * 2 * wide**3,
        limit=HALF_LIMIT,
    )(own, got, second, out_weight)


def column_block(weight, place, zlen):
    dz, dx = place
    column = lax.rem(lax.axis_index("z") + dz, zlen) * 2 + lax.rem(lax.axis_index("xh") + dx, 2)
    wide = weight.shape[0]
    return weight[:, pl.ds(pl.multiple_of(column * wide, 128), wide)]


def apply_body(zlen, counts, queries, mine, got, second, weight, out, far_top, far_low):
    core0 = core_is_first()
    rows, wide = out.shape
    limit = counts[0, counts.shape[1] - 1]
    tile = rows // 2
    for part, far_out in enumerate((far_top, far_low)):
        span = pl.ds(part * tile, tile)
        q = queries[span, :]
        a = dot(q, mine[...])
        b = dot(q, got[...])
        first_pre = jnp.where(core0, a, b)
        third_pre = jnp.where(core0, b, a)
        hidden = (first_pre / (1.0 + jnp.exp(-first_pre)) * third_pre).astype(BF)
        spot = lax.broadcasted_iota(jnp.int32, (tile, wide), 0) + part * tile
        head = jnp.where(spot < limit, dot(hidden, second[...]), 0.0).astype(BF)
        out[span, :] = head
        far_out[...] = dot(head, column_block(weight, FAR, zlen)).astype(BF)


def cross_body(zlen, x, weight, cross, same_top, same_low, hold_up, hold_down):
    half = same_top.shape[0]
    top, low = pl.ds(0, half), pl.ds(half, half)
    up = column_block(weight, CROSS_UP, zlen)
    cross[low, :] = dot(x[low, :], up).astype(BF)
    hold_up[...] = dot(x[top, :], up)
    down = column_block(weight, CROSS_DOWN, zlen)
    cross[top, :] = dot(x[top, :], down).astype(BF)
    hold_down[...] = dot(x[low, :], down)
    same = column_block(weight, SAME, zlen)
    same_top[...] = dot(x[top, :], same).astype(BF)
    same_low[...] = dot(x[low, :], same).astype(BF)


def project_body(zlen, x, weight, *outs):
    for place, out in zip(NEXT, outs):
        out[...] = dot(x[...], column_block(weight, place, zlen))


def turn(count, by):
    return [(index, (index + by) % count) for index in range(count)]


FAR = (2, 1)
SAME = (2, 0)
CROSS_UP = (1, 1)
CROSS_DOWN = (3, 1)
NEXT = ((1, 0), (3, 0), (0, 1), (0, 0))


def mixed_sum(counts, queries, new_mine, new_got, new_second, out_weight, zlen):
    rows, cols = queries.shape
    half = rows // 2
    one = 2 * rows * cols * cols

    def send(value, axis, by):
        return lax.ppermute(value, axis, turn({"z": zlen, "xh": 2}[axis], by))

    def wide(*values):
        return sum(value.astype(F32) for value in values)

    full, part = (rows, cols), (half, cols)
    head_out, far_top, far_low = call(
        functools.partial(apply_body, zlen),
        (sds(full, BF), sds(part, BF), sds(part, BF)),
        [smem()] + vmem(5),
        flops=4 * one,
        limit=24,
    )(counts, queries, new_mine, new_got, new_second, out_weight)
    far_top = send(far_top, "z", 1)
    far_low = send(far_low, "z", zlen - 1)
    cross, same_top, same_low, hold_up, hold_down = call(
        functools.partial(cross_body, zlen),
        (sds(full, BF), sds(part, BF), sds(part, BF), sds(part, F32), sds(part, F32)),
        vmem(2),
        flops=3 * one,
        limit=24,
    )(head_out, out_weight)
    cross = send(cross, "xh", 1)
    same_top = send(same_top, "z", 1)
    same_low = send(same_low, "z", zlen - 1)
    next_up, next_down, next_over, own = call(
        functools.partial(project_body, zlen),
        (sds(full, F32),) * len(NEXT),
        vmem(2),
        flops=4 * one,
        limit=24,
    )(head_out, out_weight)
    by_up = send(wide(hold_up, far_top).astype(BF), "z", 1)
    by_down = send(wide(hold_down, far_low).astype(BF), "z", zlen - 1)
    to_up = wide(next_up, jnp.concatenate([same_top, cross[half:]])).astype(BF)
    to_down = wide(next_down, jnp.concatenate([cross[:half], same_low])).astype(BF)
    from_low = send(to_up, "z", 1)
    from_high = send(to_down, "z", zlen - 1)
    over_top = send(add_rows(next_over, by_up, 0), "xh", 1)
    over_low = send(add_rows(next_over, by_down, half), "xh", 1)
    from_over = jnp.concatenate([over_top, over_low])
    return wide(own, from_low, from_high, from_over).astype(BF)


def add_rows(full, more, start):
    rows = more.shape[0]

    def body(a, b, out):
        out[...] = (a[pl.ds(start, rows), :] + b[...].astype(F32)).astype(BF)

    return call(body, sds(more.shape, BF), vmem(2), flops=1 << 24, limit=8)(full, more)


def on_device(
    keys, values, step_rates, queries, first_weight, third_weight, second_weight, out_weight,
    live_counts, ylen, zlen,
):
    first, third = first_weight[0], third_weight[0]
    swap = lambda v: lax.ppermute(v, "c", turn(2, 1))

    counts = live_counts.T
    groups, rows, _ = keys.shape
    live = jnp.arange(rows, dtype=jnp.int32)[None, None, :] < live_counts[:groups, :, None]
    scales = jnp.where(live, step_rates, 0.0)
    mine, other, half, half_other = grads(
        keys, values, scales, first_weight, third_weight, second_weight
    )
    totals = trade(spread(trade(fold(mine, swap(other), half, swap(half_other), 2 * ylen))))
    totals_got = swap(totals)
    new_mine, second, near_queries = ns_pair(totals, first, third, second_weight, queries)
    new_got = swap(new_mine)
    new_second = ns_half(totals, totals_got, second, out_weight)
    return mixed_sum(counts, near_queries, new_mine, new_got, new_second, out_weight, zlen)


def solution(mesh):
    xlen, ylen, zlen = 2, 4, 4
    split = Mesh(mesh.devices.reshape(zlen, 2, xlen, ylen, 2), HEAD + SEQ)
    in_specs = (
        P(None, SEQ, HEAD),
        P(None, SEQ, HEAD),
        P(None, HEAD, SEQ),
        P(SEQ, HEAD),
        P(HEAD, None, None),
        P(HEAD, None, None),
        P(HEAD, None, None),
        P(HEAD, None),
        P(None, SEQ),
    )

    def body(*args):
        return on_device(*args, ylen, zlen)

    return jax.shard_map(
        body, mesh=split, in_specs=in_specs, out_specs=P(SEQ, HEAD), check_vma=False
    )
```

```python
import functools

import jax
import jax.numpy as jnp
from jax import lax
from jax.experimental import pallas as pl
from jax.experimental.pallas import tpu as pltpu
from jax.sharding import Mesh
from jax.sharding import PartitionSpec as P


NS_ITERS = 3
GRADS_LIMIT = 52
PAIR_LIMIT = 30
HALF_LIMIT = 30
HEAD = ("z", "xh")
SEQ = ("xl", "y", "c")
CHIPS = ("xl", "y")


coef_a = 3.4445
coef_b = -4.775
coef_c = 2.0315
step_size = 0.5

BF = jnp.bfloat16
F32 = jnp.float32


def sds(shape, dtype):
    return jax.ShapeDtypeStruct(shape, dtype)


def vmem(count):
    return [pl.BlockSpec(memory_space=pltpu.VMEM)] * count


def smem():
    return pl.BlockSpec(memory_space=pltpu.SMEM)


def far_spec():
    return pl.BlockSpec(memory_space=pltpu.HBM)


def call(body, outs, in_specs, scratch=(), flops=0, limit=32):
    return pl.pallas_call(
        body,
        out_shape=outs,
        in_specs=in_specs,
        out_specs=jax.tree.map(lambda _: pl.BlockSpec(memory_space=pltpu.VMEM), outs),
        scratch_shapes=scratch,
        compiler_params=pltpu.CompilerParams(vmem_limit_bytes=limit << 20),
        cost_estimate=pl.CostEstimate(flops=flops, bytes_accessed=4 << 20, transcendentals=0),
    )


def dot(left, right):
    return jnp.dot(left, right, preferred_element_type=F32)


def dot_tn(left, right):
    return lax.dot_general(left, right, (((0,), (0,)), ((), ())), preferred_element_type=F32)


def dot_nt(left, right):
    return lax.dot_general(left, right, (((1,), (1,)), ((), ())), preferred_element_type=F32)


def core_is_first():
    return lax.axis_index("c") == 0


def grads_body(
    keys_h, values_h, rates, first_h, third_h, second_h,
    mine, other, half, half_other,
    keys, values, first, third, second, hidden_s, weighted_s, bm_s, bo_s, sems,
):
    core0 = core_is_first()
    groups, rows, wide = keys_h.shape
    copies = {}

    def fetch(name, source, target):
        copies[name] = pltpu.make_async_copy(source, target, sems.at[len(copies)])
        copies[name].start()

    fetch("first", first_h.at[0], first)
    fetch("k0", keys_h.at[0], keys.at[pl.ds(0, rows)])
    fetch("third", third_h.at[0], third)
    fetch("v0", values_h.at[0], values.at[pl.ds(0, rows)])
    fetch("second", second_h.at[0], second)
    for group in range(1, groups):
        fetch(f"k{group}", keys_h.at[group], keys.at[pl.ds(group * rows, rows)])
        fetch(f"v{group}", values_h.at[group], values.at[pl.ds(group * rows, rows)])

    def ready(*names):
        for name in names:
            if name in copies:
                copies.pop(name).wait()

    tile = 256
    lanes = 128
    for group in range(groups):
        for part in range(rows // tile):
            block = pl.ds(group * rows + part * tile, tile)
            ready("first", f"k{group}", "third")
            k = keys[block, :]
            first_pre = dot(k, first[...])
            third_pre = dot(k, third[...])
            ready(f"v{group}", "second")
            row = rates[group, :, pl.ds(part * tile, tile)]
            scale = jnp.broadcast_to(row, (lanes, tile)).T
            scale = jnp.concatenate([scale] * (wide // lanes), axis=1)
            weighted = (values[block, :].astype(F32) * scale).astype(BF)
            weighted_s[block, :] = weighted
            sig = 1.0 / (1.0 + jnp.exp(-first_pre))
            swish = first_pre * sig
            hidden_s[block, :] = (swish * third_pre).astype(BF)
            back = dot_nt(weighted, second[...])
            back_first = (back * third_pre * sig * (1.0 + first_pre * (1.0 - sig))).astype(BF)
            back_third = (back * swish).astype(BF)
            bm_s[block, :] = jnp.where(core0, back_first, back_third)
            bo_s[block, :] = jnp.where(core0, back_third, back_first)
    mine[...] = dot_tn(keys[...], bm_s[...]).astype(BF)
    other[...] = dot_tn(keys[...], bo_s[...]).astype(BF)
    low = wide // 2
    total = dot_tn(hidden_s[...], weighted_s[...])
    half[...] = jnp.where(core0, total[:low], total[low:]).astype(BF)
    half_other[...] = jnp.where(core0, total[low:], total[:low]).astype(BF)


def grads(keys, values, rates, first, third, second):
    groups, rows, wide = keys.shape
    total = groups * rows
    tokens = pltpu.VMEM((total, wide), BF)
    weight = pltpu.VMEM((wide, wide), BF)
    return call(
        grads_body,
        (
            sds((wide, wide), BF),
            sds((wide, wide), BF),
            sds((wide // 2, wide), BF),
            sds((wide // 2, wide), BF),
        ),
        [far_spec(), far_spec(), vmem(1)[0]] + [far_spec()] * 3,
        [tokens, tokens, weight, weight, weight]
        + [tokens] * 4
        + [pltpu.SemaphoreType.DMA((3 + 2 * groups,))],
        flops=6 * 2 * total * wide * wide,
        limit=GRADS_LIMIT,
    )(keys, values, rates, first, third, second)


def fold_body(mine, got, half, half_got, out):
    chips = out.shape[0]
    rows = mine.shape[0] // chips
    less = half.shape[0] // chips
    for index in range(chips):
        for own, more, base, size in ((mine, got, 0, rows), (half, half_got, rows, less)):
            span = pl.ds(index * size, size)
            total = own[span, :].astype(F32) + more[span, :].astype(F32)
            out[index, pl.ds(base, size), :] = total.astype(BF)


def fold(mine, got, half, half_got, chips):
    wide = mine.shape[1]
    out = sds((chips, (mine.shape[0] + half.shape[0]) // chips, wide), BF)
    return call(fold_body, out, vmem(4), flops=1 << 27, limit=10)(mine, got, half, half_got)


def spread_body(parts, out):
    total = parts[0].astype(F32)
    for index in range(1, parts.shape[0]):
        total = total + parts[index].astype(F32)
    for index in range(parts.shape[0]):
        out[index] = total.astype(BF)


def spread(parts):
    return call(spread_body, sds(parts.shape, BF), vmem(1), flops=1 << 27, limit=10)(parts)


def trade(parts):
    return lax.all_to_all(parts, CHIPS, 0, 0)


def column_spans(wide):
    return [(start, min(256, wide - start)) for start in range(0, wide, 256)]


def store_symmetric(target, lower, start, size):
    target[start:, start : start + size] = lower
    if start + size < target.shape[0]:
        target[start : start + size, start + size :] = lower[size:, :].T


def poly_step(x, out, gram_s, low_s, poly_s):
    wide = x.shape[0]
    for start, size in column_spans(wide):
        gram = dot_nt(x[start:, :], x[start : start + size, :])
        gram_s[start:, start : start + size] = gram
        store_symmetric(low_s, gram.astype(BF), start, size)
    for start, size in column_spans(wide):
        square = dot(low_s[start:, :], low_s[:, start : start + size])
        poly = coef_b * gram_s[start:, start : start + size] + coef_c * square
        store_symmetric(poly_s, poly.astype(BF), start, size)
    for start, size in column_spans(wide):
        span = slice(start, start + size)
        out[:, span] = (coef_a * x[:, span].astype(F32) + dot(poly_s[...], x[:, span])).astype(BF)


def ns_core(pieces, x_a, x_b, *scratch):
    squares = 0.0
    for load, _ in pieces:
        grad = load().astype(F32)
        squares = squares + jnp.sum(grad * grad, axis=0, keepdims=True)
    inverse = 1.0 / (jnp.sqrt(jnp.sum(squares)) + 1e-06)
    for load, span in pieces:
        x_a[span, :] = (load().astype(F32) * inverse).astype(BF)
    for _ in range(NS_ITERS):
        poly_step(x_a, x_b, *scratch)
        x_a, x_b = x_b, x_a
    return x_a


def renew(old, x_s, out):
    fresh = old + step_size * x_s[...].astype(F32)
    ratio = jnp.sqrt(jnp.mean(old * old, axis=0, keepdims=True) + 1e-06) / jnp.sqrt(
        jnp.mean(fresh * fresh, axis=0, keepdims=True) + 1e-06
    )
    out[...] = (fresh * ratio).astype(BF)


def begin(copies, sems):
    started = [
        pltpu.make_async_copy(source, target, sems.at[index])
        for index, (source, target) in enumerate(copies)
    ]
    for copy in started:
        copy.start()
    return started


def ns_pair_body(totals, first, third, second_h, queries_h, out, second, queries, full, *rest):
    work, sems = rest[:-1], rest[-1]
    copies = begin([(second_h.at[0], second), (queries_h, queries)], sems)
    chips = totals.shape[0]
    rows = out.shape[0] // chips
    pieces = [
        (functools.partial(lambda i: totals[i, pl.ds(0, rows), :], index), pl.ds(index * rows, rows))
        for index in range(chips)
    ]
    old = jnp.where(core_is_first(), first[...], third[...]).astype(F32)
    renew(old, ns_core(pieces, *work), out)
    for copy in copies:
        copy.wait()


def ns_half_body(own, got, second, _, out, full, *rest):
    work = rest[:-1]
    wide = out.shape[1]
    core0 = core_is_first()
    chips = own.shape[0]
    low = wide // 2
    rows = low // chips
    part = pl.ds(own.shape[1] - rows, rows)
    for index in range(chips):
        a = own[index, part, :].astype(F32)
        b = got[index, part, :].astype(F32)
        full[pl.ds(index * rows, rows), :] = jnp.where(core0, a, b)
        full[pl.ds(low + index * rows, rows), :] = jnp.where(core0, b, a)
    renew(second[...].astype(F32), ns_core([(lambda: full[...], slice(None))], *work), out)


def ns_scratch(wide, copies):
    return [
        pltpu.VMEM((wide, wide), F32),
        pltpu.VMEM((wide, wide), BF),
        pltpu.VMEM((wide, wide), BF),
        pltpu.VMEM((wide, wide), F32),
        pltpu.VMEM((wide, wide), BF),
        pltpu.VMEM((wide, wide), BF),
        pltpu.SemaphoreType.DMA((copies,)),
    ]


def ns_pair(totals, first, third, second, queries):
    wide = first.shape[1]
    weight = sds((wide, wide), BF)
    return call(
        ns_pair_body,
        (weight, weight, sds(queries.shape, BF)),
        vmem(3) + [far_spec()] * 2,
        ns_scratch(wide, 2),
        flops=9 * 2 * wide**3,
        limit=PAIR_LIMIT,
    )(totals, first, third, second, queries)


def ns_half(own, got, second, out_weight):
    wide = second.shape[1]
    return call(
        ns_half_body,
        sds((wide, wide), BF),
        vmem(4),
        ns_scratch(wide, 1),
        flops=9 * 2 * wide**3,
        limit=HALF_LIMIT,
    )(own, got, second, out_weight)


def column_block(weight, place, zlen):
    dz, dx = place
    column = lax.rem(lax.axis_index("z") + dz, zlen) * 2 + lax.rem(lax.axis_index("xh") + dx, 2)
    wide = weight.shape[0]
    return weight[:, pl.ds(pl.multiple_of(column * wide, 128), wide)]


def apply_body(zlen, counts, queries, mine, got, second, weight, out, far_top, far_low):
    core0 = core_is_first()
    rows, wide = out.shape
    limit = counts[0, counts.shape[1] - 1]
    tile = rows // 2
    for part, far_out in enumerate((far_top, far_low)):
        span = pl.ds(part * tile, tile)
        q = queries[span, :]
        a = dot(q, mine[...])
        b = dot(q, got[...])
        first_pre = jnp.where(core0, a, b)
        third_pre = jnp.where(core0, b, a)
        hidden = (first_pre / (1.0 + jnp.exp(-first_pre)) * third_pre).astype(BF)
        spot = lax.broadcasted_iota(jnp.int32, (tile, wide), 0) + part * tile
        head = jnp.where(spot < limit, dot(hidden, second[...]), 0.0).astype(BF)
        out[span, :] = head
        far_out[...] = dot(head, column_block(weight, FAR, zlen)).astype(BF)


def cross_body(zlen, x, weight, cross, same_top, same_low, hold_up, hold_down):
    half = same_top.shape[0]
    top, low = pl.ds(0, half), pl.ds(half, half)
    up = column_block(weight, CROSS_UP, zlen)
    cross[low, :] = dot(x[low, :], up).astype(BF)
    hold_up[...] = dot(x[top, :], up)
    down = column_block(weight, CROSS_DOWN, zlen)
    cross[top, :] = dot(x[top, :], down).astype(BF)
    hold_down[...] = dot(x[low, :], down)
    same = column_block(weight, SAME, zlen)
    same_top[...] = dot(x[top, :], same).astype(BF)
    same_low[...] = dot(x[low, :], same).astype(BF)


def project_body(zlen, x, weight, *outs):
    for place, out in zip(NEXT, outs):
        out[...] = dot(x[...], column_block(weight, place, zlen))


def turn(count, by):
    return [(index, (index + by) % count) for index in range(count)]


FAR = (2, 1)
SAME = (2, 0)
CROSS_UP = (1, 1)
CROSS_DOWN = (3, 1)
NEXT = ((1, 0), (3, 0), (0, 1), (0, 0))


def mixed_sum(counts, queries, new_mine, new_got, new_second, out_weight, zlen):
    rows, cols = queries.shape
    half = rows // 2
    one = 2 * rows * cols * cols

    def send(value, axis, by):
        return lax.ppermute(value, axis, turn({"z": zlen, "xh": 2}[axis], by))

    def wide(*values):
        return sum(value.astype(F32) for value in values)

    full, part = (rows, cols), (half, cols)
    head_out, far_top, far_low = call(
        functools.partial(apply_body, zlen),
        (sds(full, BF), sds(part, BF), sds(part, BF)),
        [smem()] + vmem(5),
        flops=4 * one,
        limit=24,
    )(counts, queries, new_mine, new_got, new_second, out_weight)
    far_top = send(far_top, "z", 1)
    far_low = send(far_low, "z", zlen - 1)
    cross, same_top, same_low, hold_up, hold_down = call(
        functools.partial(cross_body, zlen),
        (sds(full, BF), sds(part, BF), sds(part, BF), sds(part, F32), sds(part, F32)),
        vmem(2),
        flops=3 * one,
        limit=24,
    )(head_out, out_weight)
    cross = send(cross, "xh", 1)
    same_top = send(same_top, "z", 1)
    same_low = send(same_low, "z", zlen - 1)
    next_up, next_down, next_over, own = call(
        functools.partial(project_body, zlen),
        (sds(full, F32),) * len(NEXT),
        vmem(2),
        flops=4 * one,
        limit=24,
    )(head_out, out_weight)
    by_up = send(wide(hold_up, far_top).astype(BF), "z", 1)
    by_down = send(wide(hold_down, far_low).astype(BF), "z", zlen - 1)
    to_up = wide(next_up, jnp.concatenate([same_top, cross[half:]])).astype(BF)
    to_down = wide(next_down, jnp.concatenate([cross[:half], same_low])).astype(BF)
    from_low = send(to_up, "z", 1)
    from_high = send(to_down, "z", zlen - 1)
    over_top = send(add_rows(next_over, by_up, 0), "xh", 1)
    over_low = send(add_rows(next_over, by_down, half), "xh", 1)
    return finish(own, from_low, from_high, over_top, over_low)


def finish(own, low, high, over_top, over_low):
    rows, cols = own.shape
    tile = rows // 4

    def body(own, low, high, over_top, over_low, out):
        step = pl.program_id(0)
        span = pl.ds(pl.multiple_of(step * tile, tile), tile)
        near = pl.ds(pl.multiple_of((step % 2) * tile, tile), tile)
        over = jnp.where(step < 2, over_top[near, :].astype(F32), over_low[near, :].astype(F32))
        total = own[span, :] + low[span, :].astype(F32) + high[span, :].astype(F32) + over
        out[...] = total.astype(BF)

    return pl.pallas_call(
        body,
        out_shape=sds((rows, cols), BF),
        grid=(4,),
        in_specs=vmem(5),
        out_specs=pl.BlockSpec((tile, cols), lambda step: (step, 0)),
        compiler_params=pltpu.CompilerParams(vmem_limit_bytes=16 << 20),
        cost_estimate=pl.CostEstimate(flops=1 << 24, bytes_accessed=1 << 20, transcendentals=0),
    )(own, low, high, over_top, over_low)


def add_rows(full, more, start):
    rows = more.shape[0]

    def body(a, b, out):
        out[...] = (a[pl.ds(start, rows), :] + b[...].astype(F32)).astype(BF)

    return call(body, sds(more.shape, BF), vmem(2), flops=1 << 24, limit=8)(full, more)


def on_device(
    keys, values, step_rates, queries, first_weight, third_weight, second_weight, out_weight,
    live_counts, ylen, zlen,
):
    first, third = first_weight[0], third_weight[0]
    swap = lambda v: lax.ppermute(v, "c", turn(2, 1))

    counts = live_counts.T
    rates = jnp.pad(step_rates, ((0, live_counts.shape[0] - step_rates.shape[0]), (0, 0), (0, 0)))
    spots = lax.broadcasted_iota(jnp.int32, rates.shape, 2)
    scales = jnp.where(spots < live_counts[:, :, None], rates, 0.0)
    mine, other, half, half_other = grads(
        keys, values, scales, first_weight, third_weight, second_weight
    )
    totals = trade(spread(trade(fold(mine, swap(other), half, swap(half_other), 2 * ylen))))
    totals_got = swap(totals)
    new_mine, second, near_queries = ns_pair(totals, first, third, second_weight, queries)
    new_got = swap(new_mine)
    new_second = ns_half(totals, totals_got, second, out_weight)
    return mixed_sum(counts, near_queries, new_mine, new_got, new_second, out_weight, zlen)


def solution(mesh):
    xlen, ylen, zlen = 2, 4, 4
    split = Mesh(mesh.devices.reshape(zlen, 2, xlen, ylen, 2), HEAD + SEQ)
    in_specs = (
        P(None, SEQ, HEAD),
        P(None, SEQ, HEAD),
        P(None, HEAD, SEQ),
        P(SEQ, HEAD),
        P(HEAD, None, None),
        P(HEAD, None, None),
        P(HEAD, None, None),
        P(HEAD, None),
        P(None, SEQ),
    )

    def body(*args):
        return on_device(*args, ylen, zlen)

    return jax.shard_map(
        body, mesh=split, in_specs=in_specs, out_specs=P(SEQ, HEAD), check_vma=False
    )
```

```python
import functools

import jax
import jax.numpy as jnp
from jax import lax
from jax.experimental import pallas as pl
from jax.experimental.pallas import tpu as pltpu
from jax.sharding import Mesh
from jax.sharding import PartitionSpec as P


NS_ITERS = 3
GRADS_LIMIT = 52
PAIR_LIMIT = 30
HALF_LIMIT = 30
HEAD = ("z", "xh")
SEQ = ("xl", "y", "c")
CHIPS = ("xl", "y")


coef_a = 3.4445
coef_b = -4.775
coef_c = 2.0315
step_size = 0.5

BF = jnp.bfloat16
F32 = jnp.float32


def sds(shape, dtype):
    return jax.ShapeDtypeStruct(shape, dtype)


def vmem(count):
    return [pl.BlockSpec(memory_space=pltpu.VMEM)] * count


def smem():
    return pl.BlockSpec(memory_space=pltpu.SMEM)


def far_spec():
    return pl.BlockSpec(memory_space=pltpu.HBM)


def call(body, outs, in_specs, scratch=(), flops=0, limit=32):
    return pl.pallas_call(
        body,
        out_shape=outs,
        in_specs=in_specs,
        out_specs=jax.tree.map(lambda _: pl.BlockSpec(memory_space=pltpu.VMEM), outs),
        scratch_shapes=scratch,
        compiler_params=pltpu.CompilerParams(vmem_limit_bytes=limit << 20),
        cost_estimate=pl.CostEstimate(flops=flops, bytes_accessed=4 << 20, transcendentals=0),
    )


def dot(left, right):
    return jnp.dot(left, right, preferred_element_type=F32)


def dot_tn(left, right):
    return lax.dot_general(left, right, (((0,), (0,)), ((), ())), preferred_element_type=F32)


def dot_nt(left, right):
    return lax.dot_general(left, right, (((1,), (1,)), ((), ())), preferred_element_type=F32)


def core_is_first():
    return lax.axis_index("c") == 0


def grads_body(
    keys_h, values_h, rates, first_h, third_h, second_h,
    mine, other, half, half_other,
    keys, values, first, third, second, hidden_s, weighted_s, bm_s, bo_s, sems,
):
    core0 = core_is_first()
    groups, rows, wide = keys_h.shape
    copies = {}

    def fetch(name, source, target):
        copies[name] = pltpu.make_async_copy(source, target, sems.at[len(copies)])
        copies[name].start()

    fetch("first", first_h.at[0], first)
    fetch("k0", keys_h.at[0], keys.at[pl.ds(0, rows)])
    fetch("third", third_h.at[0], third)
    fetch("v0", values_h.at[0], values.at[pl.ds(0, rows)])
    fetch("second", second_h.at[0], second)
    for group in range(1, groups):
        fetch(f"k{group}", keys_h.at[group], keys.at[pl.ds(group * rows, rows)])
        fetch(f"v{group}", values_h.at[group], values.at[pl.ds(group * rows, rows)])

    def ready(*names):
        for name in names:
            if name in copies:
                copies.pop(name).wait()

    tile = 256
    lanes = 128
    for group in range(groups):
        for part in range(rows // tile):
            block = pl.ds(group * rows + part * tile, tile)
            ready("first", f"k{group}", "third")
            k = keys[block, :]
            first_pre = dot(k, first[...])
            third_pre = dot(k, third[...])
            ready(f"v{group}", "second")
            row = rates[group, :, pl.ds(part * tile, tile)]
            scale = jnp.broadcast_to(row, (lanes, tile)).T
            scale = jnp.concatenate([scale] * (wide // lanes), axis=1)
            weighted = (values[block, :].astype(F32) * scale).astype(BF)
            weighted_s[block, :] = weighted
            sig = 1.0 / (1.0 + jnp.exp(-first_pre))
            swish = first_pre * sig
            hidden_s[block, :] = (swish * third_pre).astype(BF)
            back = dot_nt(weighted, second[...])
            back_first = (back * third_pre * sig * (1.0 + first_pre * (1.0 - sig))).astype(BF)
            back_third = (back * swish).astype(BF)
            bm_s[block, :] = jnp.where(core0, back_first, back_third)
            bo_s[block, :] = jnp.where(core0, back_third, back_first)
    mine[...] = dot_tn(keys[...], bm_s[...]).astype(BF)
    other[...] = dot_tn(keys[...], bo_s[...]).astype(BF)
    low = wide // 2
    total = dot_tn(hidden_s[...], weighted_s[...])
    half[...] = jnp.where(core0, total[:low], total[low:]).astype(BF)
    half_other[...] = jnp.where(core0, total[low:], total[:low]).astype(BF)


def grads(keys, values, rates, first, third, second):
    groups, rows, wide = keys.shape
    total = groups * rows
    tokens = pltpu.VMEM((total, wide), BF)
    weight = pltpu.VMEM((wide, wide), BF)
    return call(
        grads_body,
        (
            sds((wide, wide), BF),
            sds((wide, wide), BF),
            sds((wide // 2, wide), BF),
            sds((wide // 2, wide), BF),
        ),
        [far_spec(), far_spec(), vmem(1)[0]] + [far_spec()] * 3,
        [tokens, tokens, weight, weight, weight]
        + [tokens] * 4
        + [pltpu.SemaphoreType.DMA((3 + 2 * groups,))],
        flops=6 * 2 * total * wide * wide,
        limit=GRADS_LIMIT,
    )(keys, values, rates, first, third, second)


def fold_body(mine, got, half, half_got, out):
    chips = out.shape[0]
    rows = mine.shape[0] // chips
    less = half.shape[0] // chips
    for index in range(chips):
        for own, more, base, size in ((mine, got, 0, rows), (half, half_got, rows, less)):
            span = pl.ds(index * size, size)
            total = own[span, :].astype(F32) + more[span, :].astype(F32)
            out[index, pl.ds(base, size), :] = total.astype(BF)


def fold(mine, got, half, half_got, chips):
    wide = mine.shape[1]
    out = sds((chips, (mine.shape[0] + half.shape[0]) // chips, wide), BF)
    return call(fold_body, out, vmem(4), flops=1 << 27, limit=10)(mine, got, half, half_got)


def spread_body(parts, out):
    total = parts[0].astype(F32)
    for index in range(1, parts.shape[0]):
        total = total + parts[index].astype(F32)
    for index in range(parts.shape[0]):
        out[index] = total.astype(BF)


def spread(parts):
    return call(spread_body, sds(parts.shape, BF), vmem(1), flops=1 << 27, limit=10)(parts)


def trade(parts):
    return lax.all_to_all(parts, CHIPS, 0, 0)


def column_spans(wide):
    return [(start, min(256, wide - start)) for start in range(0, wide, 256)]


def store_symmetric(target, lower, start, size):
    target[start:, start : start + size] = lower
    if start + size < target.shape[0]:
        target[start : start + size, start + size :] = lower[size:, :].T


def poly_step(x, out, gram_s, low_s, poly_s):
    wide = x.shape[0]
    for start, size in column_spans(wide):
        gram = dot_nt(x[start:, :], x[start : start + size, :])
        gram_s[start:, start : start + size] = gram
        store_symmetric(low_s, gram.astype(BF), start, size)
    for start, size in column_spans(wide):
        square = dot(low_s[start:, :], low_s[:, start : start + size])
        poly = coef_b * gram_s[start:, start : start + size] + coef_c * square
        store_symmetric(poly_s, poly.astype(BF), start, size)
    for start, size in column_spans(wide):
        span = slice(start, start + size)
        out[:, span] = (coef_a * x[:, span].astype(F32) + dot(poly_s[...], x[:, span])).astype(BF)


def ns_core(pieces, x_a, x_b, *scratch):
    squares = 0.0
    for load, _ in pieces:
        grad = load().astype(F32)
        squares = squares + jnp.sum(grad * grad, axis=0, keepdims=True)
    inverse = 1.0 / (jnp.sqrt(jnp.sum(squares)) + 1e-06)
    for load, span in pieces:
        x_a[span, :] = (load().astype(F32) * inverse).astype(BF)
    for _ in range(NS_ITERS):
        poly_step(x_a, x_b, *scratch)
        x_a, x_b = x_b, x_a
    return x_a


def renew(old, x_s, out):
    fresh = old + step_size * x_s[...].astype(F32)
    ratio = jnp.sqrt(jnp.mean(old * old, axis=0, keepdims=True) + 1e-06) / jnp.sqrt(
        jnp.mean(fresh * fresh, axis=0, keepdims=True) + 1e-06
    )
    out[...] = (fresh * ratio).astype(BF)


def begin(copies, sems):
    started = [
        pltpu.make_async_copy(source, target, sems.at[index])
        for index, (source, target) in enumerate(copies)
    ]
    for copy in started:
        copy.start()
    return started


def ns_pair_body(totals, first, third, second_h, queries_h, out, second, queries, full, *rest):
    work, sems = rest[:-1], rest[-1]
    copies = begin([(second_h.at[0], second), (queries_h, queries)], sems)
    chips = totals.shape[0]
    rows = out.shape[0] // chips
    pieces = [
        (functools.partial(lambda i: totals[i, pl.ds(0, rows), :], index), pl.ds(index * rows, rows))
        for index in range(chips)
    ]
    old = jnp.where(core_is_first(), first[...], third[...]).astype(F32)
    renew(old, ns_core(pieces, *work), out)
    for copy in copies:
        copy.wait()


def ns_half_body(own, got, second, _, out, full, *rest):
    work = rest[:-1]
    wide = out.shape[1]
    core0 = core_is_first()
    chips = own.shape[0]
    low = wide // 2
    rows = low // chips
    part = pl.ds(own.shape[1] - rows, rows)

    def piece(index, upper):
        a = own[index, part, :].astype(F32)
        b = got[index, part, :].astype(F32)
        return jnp.where(core0, a, b) if upper else jnp.where(core0, b, a)

    pieces = [
        (functools.partial(piece, index, base == 0), pl.ds(base + index * rows, rows))
        for base in (0, low)
        for index in range(chips)
    ]
    renew(second[...].astype(F32), ns_core(pieces, *work), out)


def ns_scratch(wide, copies):
    return [
        pltpu.VMEM((wide, wide), F32),
        pltpu.VMEM((wide, wide), BF),
        pltpu.VMEM((wide, wide), BF),
        pltpu.VMEM((wide, wide), F32),
        pltpu.VMEM((wide, wide), BF),
        pltpu.VMEM((wide, wide), BF),
        pltpu.SemaphoreType.DMA((copies,)),
    ]


def ns_pair(totals, first, third, second, queries):
    wide = first.shape[1]
    weight = sds((wide, wide), BF)
    return call(
        ns_pair_body,
        (weight, weight, sds(queries.shape, BF)),
        vmem(3) + [far_spec()] * 2,
        ns_scratch(wide, 2),
        flops=9 * 2 * wide**3,
        limit=PAIR_LIMIT,
    )(totals, first, third, second, queries)


def ns_half(own, got, second, out_weight):
    wide = second.shape[1]
    return call(
        ns_half_body,
        sds((wide, wide), BF),
        vmem(4),
        ns_scratch(wide, 1),
        flops=9 * 2 * wide**3,
        limit=HALF_LIMIT,
    )(own, got, second, out_weight)


def column_block(weight, place, zlen):
    dz, dx = place
    column = lax.rem(lax.axis_index("z") + dz, zlen) * 2 + lax.rem(lax.axis_index("xh") + dx, 2)
    wide = weight.shape[0]
    return weight[:, pl.ds(pl.multiple_of(column * wide, 128), wide)]


def apply_body(zlen, counts, queries, mine, got, second, weight, out, far_top, far_low):
    core0 = core_is_first()
    rows, wide = out.shape
    limit = counts[0, counts.shape[1] - 1]
    tile = rows // 2
    for part, far_out in enumerate((far_top, far_low)):
        span = pl.ds(part * tile, tile)
        q = queries[span, :]
        a = dot(q, mine[...])
        b = dot(q, got[...])
        first_pre = jnp.where(core0, a, b)
        third_pre = jnp.where(core0, b, a)
        hidden = (first_pre / (1.0 + jnp.exp(-first_pre)) * third_pre).astype(BF)
        spot = lax.broadcasted_iota(jnp.int32, (tile, wide), 0) + part * tile
        head = jnp.where(spot < limit, dot(hidden, second[...]), 0.0).astype(BF)
        out[span, :] = head
        far_out[...] = dot(head, column_block(weight, FAR, zlen)).astype(BF)


def cross_body(zlen, x, weight, cross, same_top, same_low, hold_up, hold_down):
    half = same_top.shape[0]
    top, low = pl.ds(0, half), pl.ds(half, half)
    up = column_block(weight, CROSS_UP, zlen)
    cross[low, :] = dot(x[low, :], up).astype(BF)
    hold_up[...] = dot(x[top, :], up)
    down = column_block(weight, CROSS_DOWN, zlen)
    cross[top, :] = dot(x[top, :], down).astype(BF)
    hold_down[...] = dot(x[low, :], down)
    same = column_block(weight, SAME, zlen)
    same_top[...] = dot(x[top, :], same).astype(BF)
    same_low[...] = dot(x[low, :], same).astype(BF)


def project_body(zlen, x, weight, *outs):
    for place, out in zip(NEXT, outs):
        out[...] = dot(x[...], column_block(weight, place, zlen))


def turn(count, by):
    return [(index, (index + by) % count) for index in range(count)]


FAR = (2, 1)
SAME = (2, 0)
CROSS_UP = (1, 1)
CROSS_DOWN = (3, 1)
NEXT = ((1, 0), (3, 0), (0, 1), (0, 0))


def mixed_sum(counts, queries, new_mine, new_got, new_second, out_weight, zlen):
    rows, cols = queries.shape
    half = rows // 2
    one = 2 * rows * cols * cols

    def send(value, axis, by):
        return lax.ppermute(value, axis, turn({"z": zlen, "xh": 2}[axis], by))

    def wide(*values):
        return sum(value.astype(F32) for value in values)

    full, part = (rows, cols), (half, cols)
    head_out, far_top, far_low = call(
        functools.partial(apply_body, zlen),
        (sds(full, BF), sds(part, BF), sds(part, BF)),
        [smem()] + vmem(5),
        flops=4 * one,
        limit=24,
    )(counts, queries, new_mine, new_got, new_second, out_weight)
    far_top = send(far_top, "z", 1)
    far_low = send(far_low, "z", zlen - 1)
    cross, same_top, same_low, hold_up, hold_down = call(
        functools.partial(cross_body, zlen),
        (sds(full, BF), sds(part, BF), sds(part, BF), sds(part, F32), sds(part, F32)),
        vmem(2),
        flops=3 * one,
        limit=24,
    )(head_out, out_weight)
    cross = send(cross, "xh", 1)
    same_top = send(same_top, "z", 1)
    same_low = send(same_low, "z", zlen - 1)
    next_up, next_down, next_over, own = call(
        functools.partial(project_body, zlen),
        (sds(full, F32),) * len(NEXT),
        vmem(2),
        flops=4 * one,
        limit=24,
    )(head_out, out_weight)
    by_up = send(wide(hold_up, far_top).astype(BF), "z", 1)
    by_down = send(wide(hold_down, far_low).astype(BF), "z", zlen - 1)
    to_up = wide(next_up, jnp.concatenate([same_top, cross[half:]])).astype(BF)
    to_down = wide(next_down, jnp.concatenate([cross[:half], same_low])).astype(BF)
    from_low = send(to_up, "z", 1)
    from_high = send(to_down, "z", zlen - 1)
    over_top = send(add_rows(next_over, by_up, 0), "xh", 1)
    over_low = send(add_rows(next_over, by_down, half), "xh", 1)
    from_over = jnp.concatenate([over_top, over_low])
    return wide(own, from_low, from_high, from_over).astype(BF)


def add_rows(full, more, start):
    rows = more.shape[0]

    def body(a, b, out):
        out[...] = (a[pl.ds(start, rows), :] + b[...].astype(F32)).astype(BF)

    return call(body, sds(more.shape, BF), vmem(2), flops=1 << 24, limit=8)(full, more)


def on_device(
    keys, values, step_rates, queries, first_weight, third_weight, second_weight, out_weight,
    live_counts, ylen, zlen,
):
    first, third = first_weight[0], third_weight[0]
    swap = lambda v: lax.ppermute(v, "c", turn(2, 1))

    counts = live_counts.T
    rates = jnp.pad(step_rates, ((0, live_counts.shape[0] - step_rates.shape[0]), (0, 0), (0, 0)))
    spots = lax.broadcasted_iota(jnp.int32, rates.shape, 2)
    scales = jnp.where(spots < live_counts[:, :, None], rates, 0.0)
    mine, other, half, half_other = grads(
        keys, values, scales, first_weight, third_weight, second_weight
    )
    totals = trade(spread(trade(fold(mine, swap(other), half, swap(half_other), 2 * ylen))))
    totals_got = swap(totals)
    new_mine, second, near_queries = ns_pair(totals, first, third, second_weight, queries)
    new_got = swap(new_mine)
    new_second = ns_half(totals, totals_got, second, out_weight)
    return mixed_sum(counts, near_queries, new_mine, new_got, new_second, out_weight, zlen)


def solution(mesh):
    xlen, ylen, zlen = 2, 4, 4
    split = Mesh(mesh.devices.reshape(zlen, 2, xlen, ylen, 2), HEAD + SEQ)
    in_specs = (
        P(None, SEQ, HEAD),
        P(None, SEQ, HEAD),
        P(None, HEAD, SEQ),
        P(SEQ, HEAD),
        P(HEAD, None, None),
        P(HEAD, None, None),
        P(HEAD, None, None),
        P(HEAD, None),
        P(None, SEQ),
    )

    def body(*args):
        return on_device(*args, ylen, zlen)

    return jax.shard_map(
        body, mesh=split, in_specs=in_specs, out_specs=P(SEQ, HEAD), check_vma=False
    )
```
